128 devices in a mesh: gx: 16 (over y, x), gy: 2 (over core), gz: 4 (over z).
Axes of the slice: x: 4, y: 4, z: 4, core: 2. Of those that a mesh axis runs over, the one named last changes fastest.
Arguments:
- potential: float32 [960, 120, 512], P('gx', 'gy', 'gz'), may hold values from -6 to 6
- frag_root: int32 [3, 512], P(None, ('gx', 'gy', 'gz')), may hold values from 0 to 959, as said below
Outputs:
- frag_fields: float32 [512, 110592], P(('gx', 'gy', 'gz'))
The draws below stay inside these ranges and needn't reach their ends.
Inputs may be any that keep to these rules, and one draw needn't show every extreme that they name: `frag_root`: fragment f is held by the device of linear index f // 4 (gx slowest). Along each dimension the box's first cell is the start of a block plus an offset in [-34, B - 34), B being that dimension's cells of one device. Along y and z that block is the holding device's own; along x it is the block of some device with the same gy and gz index, the anchor. Every anchor of a device supplies exactly 1 of its fragments.
All inputs are finite; a program needn't handle non-finite values.
Results may differ from the reference program's by a relative error of at most 0.00007.
Values sent between devices are 32-bit elements; how exact they have to be, the bound alone decides.
A program may use at most 320 MiB of HBM per device.

```python
import math
import jax
import jax.numpy as jnp
from jax import lax

G = 48
CAP = 1
SLOTS = 4
BX = 60
BY = 60
BZ = 128
BOX = 68
HALO = 34
NX = 960
NY = 120
NZ = 512
N_GX = 16
N_GY = 2
N_GZ = 4


def draw_frag_root(key, part):
    subkeys = jax.random.split(jax.random.fold_in(key, 17), 6)
    devices = N_GX * N_GY * N_GZ
    pair_count = SLOTS // CAP
    favour = jax.random.randint(subkeys[0], (N_GX,), 0, 4) * 300
    jitter = jax.random.randint(subkeys[1], (devices, N_GX), 0, 1000)
    scores = (jitter + favour[None, :]) * N_GX + jnp.arange(N_GX, dtype=jnp.int32)[None, :]
    dummy_values, picked = lax.top_k(scores, pair_count)
    listed = jnp.repeat(picked.astype(jnp.int32), CAP, axis=1)
    shuffle_keys = jax.random.randint(subkeys[2], (devices, SLOTS), 0, 1000) * SLOTS + jnp.arange(SLOTS, dtype=jnp.int32)[None, :]
    shuffled = jnp.argsort(shuffle_keys, axis=1)
    anchors = jnp.take_along_axis(listed, shuffled, axis=1).reshape(-1)
    device = jnp.arange(devices * SLOTS, dtype=jnp.int32) // SLOTS
    row_y = device // N_GZ % N_GY
    row_z = device % N_GZ
    lowest = -HALO
    offset_x = jax.random.randint(subkeys[3], (devices * SLOTS,), lowest, BX - HALO)
    offset_y = jax.random.randint(subkeys[4], (devices * SLOTS,), lowest, BY - HALO)
    offset_z = jax.random.randint(subkeys[5], (devices * SLOTS,), lowest, BZ - HALO)
    offset_x = offset_x.at[0].set(lowest).at[1].set(BX - HALO - 1)
    offset_y = offset_y.at[0].set(lowest).at[1].set(BY - HALO - 1)
    offset_z = offset_z.at[0].set(lowest).at[1].set(BZ - HALO - 1)
    root_x = jnp.mod(anchors * BX + offset_x, BX * N_GX)
    root_y = jnp.mod(row_y * BY + offset_y, BY * N_GY)
    root_z = jnp.mod(row_z * BZ + offset_z, BZ * N_GZ)
    return jnp.stack([root_x, root_y, root_z]).astype(jnp.int32)


def steps_of(key, dims, pieces, smallest, top_value):
    level = 1.0
    for dim, shards_of in pieces:
        steps = jax.random.uniform(jax.random.fold_in(jax.random.fold_in(key, 6), dim), (shards_of,), jnp.float32, smallest / len(pieces), top_value / len(pieces))
        level = level * jnp.repeat(jnp.exp(steps), dims[dim] // shards_of).reshape((-1,) + (1,) * (len(dims) - 1 - dim))
    return level


def scatter_about(rng, dims, scale, most, shards=(), kind=jnp.bfloat16):
    array = scale * jax.random.normal(rng, dims, jnp.float32)
    if shards:
        array = array * steps_of(rng, dims, shards, -0.22, 0.18)
    return jnp.clip(array, -most, most).astype(kind)


def setup_inputs(seed: int = 0) -> dict:
    splits = jax.random.split(jax.random.key(seed), 3)
    potential = scatter_about(splits[0], (NX, NY, NZ), 1.0, 6.0, ((0, 16), (1, 2), (2, 4)), jnp.float32)
    frag_root = draw_frag_root(jax.random.fold_in(splits[2], 71), 0)
    return {"potential": potential, "frag_root": frag_root}


def interp_table(points, cells):
    row_index = jnp.arange(points, dtype=jnp.int32)[:, None]
    col_index = jnp.arange(cells, dtype=jnp.int32)[None, :]
    offset = row_index * cells - col_index * points
    period = points * cells
    summed = jnp.ones((points, cells), jnp.float32)
    for harmonic in range(1, points // 2):
        phase_angle = jnp.mod(harmonic * offset, period).astype(jnp.float32)
        summed = summed + 2.0 * jnp.cos((2.0 * math.pi / period) * phase_angle)
    return summed / cells


def refine(window, matrix):
    highest = lax.Precision.HIGHEST
    step_x = jnp.einsum('ax,xyz->ayz', matrix, window, precision=highest)
    step_y = jnp.einsum('by,ayz->abz', matrix, step_x, precision=highest)
    step_z = jnp.einsum('cz,abz->abc', matrix, step_y, precision=highest)
    return step_z.reshape(-1)


def reference(potential, frag_root):
    matrix = interp_table(G, BOX)
    wrapped = jnp.pad(potential, ((0, BOX), (0, BOX), (0, BOX)), mode="wrap")

    def single(corner):
        window = lax.dynamic_slice(wrapped, (corner[0], corner[1], corner[2]), (BOX, BOX, BOX))
        return refine(window, matrix)

    return lax.map(single, frag_root.T.astype(jnp.int32))
```

```python
import functools

import jax
import jax.numpy as jnp
import numpy as np
from jax import lax
from jax.experimental import pallas as pl
from jax.experimental.pallas import tpu as pltpu
from jax.sharding import PartitionSpec as P

MESH = pl.DeviceIdType.MESH
G = 48
BOX = 68
HALO = 34
BX = 60
BY = 60
BZ = 128
NX = 960
NY = 120
NZ = 512
GX = 16
SLOTS = 4
EXT = 128
YL = 128
FLAT = 864
SX = 72
LEFT = 12
OWN = 19
PACKS = LEFT + OWN + LEFT
F32 = jnp.float32
BF16 = jnp.bfloat16


def interp_matrix():
    a = np.arange(G)[:, None]
    x = np.arange(BOX)[None, :]
    total = np.ones((G, BOX))
    for k in range(1, G // 2):
        total = total + 2.0 * np.cos(2.0 * np.pi * k * (a / G - x / BOX))
    return (total / BOX).astype(np.float32)


def tables():
    m = interp_matrix()
    ytab = np.zeros((248, 128), np.float32)
    for j in range(248):
        if j % NY < BOX:
            ytab[j, :G] = m[:, j % NY]
    ztab = np.zeros((512, 128), np.float32)
    for j in range(512):
        if j % 256 < BOX:
            ztab[j, :G] = m[:, j % 256]
    mx = np.zeros((G, SX), np.float32)
    mx[:, :BOX] = m
    return ytab, ztab, mx


def split(v):
    hi = v.astype(BF16)
    return hi, (v - hi.astype(F32)).astype(BF16)


def dot(a, b):
    return jnp.dot(a, b, preferred_element_type=F32)


def kernel(
    pot, root, ytab, ztab, mxt, out,
    roots, roots_s, xr, zsend, zrecv, ehi, elo, w_ref, my_ref, s_ref, send, recv,
    root_send, root_recv, local_sem, own_sem, x_send, x_recv, xd_send, xd_recv,
    z_send, z_recv, zd_send, zd_recv, f_send, f_recv,
):
    me = lax.axis_index("gx")
    core = lax.axis_index("gy")
    plane = lax.axis_index("gz")
    my_y, my_x = me // 4, me % 4

    def line(g):
        return {"gx": g, "gy": core, "gz": plane}

    def shifted(k):
        return ((my_y + k // 4) % 4) * 4 + (my_x + k % 4) % 4

    nxt, prv = (me + 1) % GX, (me + GX - 1) % GX
    partner = {"gx": me, "gy": 1 - core, "gz": plane}
    z_up = {"gx": me, "gy": core, "gz": (plane + 1) % 4}
    z_down = {"gx": me, "gy": core, "gz": (plane + 3) % 4}

    barrier = pltpu.get_barrier_semaphore()
    for d in (partner, z_up, z_down):
        pl.semaphore_signal(barrier, inc=1, device_id=d, device_id_type=MESH)

    @pl.loop(1, GX)
    def _(k):
        pl.semaphore_signal(barrier, inc=1, device_id=line(shifted(k)), device_id_type=MESH)

    pl.semaphore_wait(barrier, GX + 2)

    mine = pl.ds(pl.multiple_of(core * 64, 64), BY)
    mine64 = pl.ds(pl.multiple_of(core * 64, 64), 64)

    def remote(src, dst, ssem, rsem, to):
        return pltpu.make_async_remote_copy(
            src_ref=src, dst_ref=dst, send_sem=ssem, recv_sem=rsem, device_id=to, device_id_type=MESH
        )

    x_parts = ((26, 0, 18, nxt), (0, 94, 16, prv), (44, 18, 16, nxt), (16, 110, 18, prv))
    x_copies = [
        remote(pot.at[pl.ds(s, n)], xr.at[pl.ds(e, n), mine], x_send.at[i], x_recv.at[i], line(to))
        for i, (s, e, n, to) in enumerate(x_parts)
    ]
    def root_copy(k):
        return remote(root, roots.at[k], root_send.at[k], root_recv.at[k], line(shifted(k)))

    @pl.loop(1, GX)
    def _(k):
        root_copy(k).start()

    for c in x_copies:
        c.start()
    local = pltpu.make_async_copy(pot, xr.at[pl.ds(HALO, BX), mine], local_sem.at[0])
    local.start()
    own_d2d = remote(pot, xr.at[pl.ds(HALO, BX), mine], own_sem.at[0], own_sem.at[1], partner)
    own_d2d.start()
    roots[0] = root[...]

    local.wait()
    own_d2d.wait_recv()

    @pl.loop(0, EXT)
    def _(x):
        xr[x, 60:64, :] = jnp.zeros((4, 128), F32)
        xr[x, 124:128, :] = jnp.zeros((4, 128), F32)

    lane = lax.broadcasted_iota(jnp.int32, (64, 128), 1)

    def pack(first, count, slab):
        @pl.loop(0, count)
        def _(p):
            x = slab + 3 * p
            up = jnp.zeros((64, 128), F32)
            down = jnp.zeros((64, 128), F32)
            for j in range(3):
                v = xr[x + j, mine64, :]
                low = 94 - 34 * j
                up = jnp.where((lane >= low) & (lane < low + 34), pltpu.roll(v, (128 - 34 * j) % 128, 1), up)
                down = jnp.where((lane >= 34 * j) & (lane < 34 * j + 34), pltpu.roll(v, 34 * j, 1), down)
            zsend[0, first + p] = up
            zsend[1, first + p] = down

    def z_copies(i, first, count):
        rows = pl.ds(first, count)
        return [
            remote(zsend.at[d, rows], zrecv.at[d, rows, mine64], z_send.at[i, d], z_recv.at[i, d], to)
            for d, to in enumerate((z_up, z_down))
        ]

    def z_relays(i, first, count):
        rows = pl.ds(first, count)
        return [
            remote(zrecv.at[d, rows, mine64], zrecv.at[d, rows, mine64], zd_send.at[i, d], zd_recv.at[i, d], partner)
            for d in range(2)
        ]

    def x_relay(i):
        _, e, n, _ = x_parts[i]
        return remote(xr.at[pl.ds(e, n), mine], xr.at[pl.ds(e, n), mine], xd_send.at[i], xd_recv.at[i], partner)

    lane_y = lax.broadcasted_iota(jnp.int32, (YL, 128), 1)

    def convert(first, count, slab):
        @pl.loop(0, count)
        def _(p):
            below = zrecv[0, first + p]
            above = zrecv[1, first + p]
            for j in range(3):
                x = slab + 3 * p + j
                v = xr[x]
                h, l = split(v)
                ehi[x, :, 0:128] = h
                elo[x, :, 0:128] = l
                edge = jnp.where(
                    lane_y < 34,
                    pltpu.roll(above, (128 - 34 * j) % 128, 1),
                    jnp.where(lane_y >= 94, pltpu.roll(below, 34 * j, 1), 0.0),
                )
                h, l = split(edge)
                ehi[x, :, 128:256] = h
                elo[x, :, 128:256] = l

    z_parts = ((0, OWN, 36), (OWN, 6, 0), (OWN + 6, 6, 92), (OWN + 12, 6, 18), (OWN + 18, 6, 110))
    z_all = [z_copies(i, f, n) for i, (f, n, _) in enumerate(z_parts)]
    relays = [z_relays(i, f, n) for i, (f, n, _) in enumerate(z_parts)]
    x_relays = [x_relay(i) for i in range(4)]

    def z_arrived(i):
        for d in range(2):
            z_all[i][d].wait_recv()
            relays[i][d].start()

    pack(*z_parts[0])
    for c in z_all[0]:
        c.start()
    for i in range(4):
        x_copies[i].wait_recv()
        x_relays[i].start()
        pack(*z_parts[i + 1])
        for c in z_all[i + 1]:
            c.start()
        if i == 2:
            z_arrived(0)
    @pl.loop(1, GX)
    def _(k):
        root_copy(k).wait_recv()

    pltpu.sync_copy(roots, roots_s)
    s_ref[...] = jnp.zeros(s_ref.shape, F32)
    for i in range(4):
        x_relays[i].wait_recv()
    for i in range(5):
        if i:
            z_arrived(i)
        if i >= 1:
            for d in range(2):
                relays[i - 1][d].wait_recv()
            convert(*z_parts[i - 1])
    for d in range(2):
        relays[4][d].wait_recv()
    convert(*z_parts[4])

    mx = mxt[...]
    roll_lane = lax.broadcasted_iota(jnp.int32, (SX, 128), 1)

    def f_copy(k):
        return remote(send.at[k], recv.at[k], f_send.at[k], f_recv.at[k], line(shifted(k)))

    def field(k, dest):
        back = ((4 - k // 4) % 4) * 4 + (4 - k % 4) % 4
        rx, ry, rz = jnp.int32(0), jnp.int32(0), jnp.int32(0)
        for s in range(SLOTS):
            fx = roots_s[back, 0, s]
            mine_too = (fx + HALO) % NX // BX == me
            rx = jnp.where(mine_too, fx, rx)
            ry = jnp.where(mine_too, roots_s[back, 1, s], ry)
            rz = jnp.where(mine_too, roots_s[back, 2, s], rz)
        sx = jnp.minimum((rx + HALO - me * BX + NX) % NX, BX - 1)
        sy = ry
        sz = (rz - plane * BZ + NZ) % 256
        my_t = jnp.concatenate([ytab[pl.ds(NY - sy, 64), :], ytab[pl.ds(NY + BY - sy, 64), :]], axis=0)
        my = my_t.T[0:G, :]
        my_hi, my_lo = split(my)
        my_ref[...] = jnp.concatenate([my_hi, my_lo], axis=0)
        z_hi, z_lo = split(ztab[pl.ds(256 - sz, 256), :])
        w_ref[:, 0:128] = z_hi
        w_ref[:, 128:256] = z_lo

        @pl.loop(0, BOX // 4)
        def _(g):
            both = my_ref[...]
            parts = []
            for j in range(4):
                x = sx + 4 * g + j
                t = dot(both, ehi[x])
                parts.append(t[:G] + t[G:] + dot(both[:G], elo[x]))
            hi, lo = split(jnp.concatenate(parts, axis=0))
            q = dot(hi, w_ref[...])
            t = q[:, :128] + q[:, 128:] + dot(lo, w_ref[:, 0:128])
            for j in range(4):
                s_ref[pl.ds(4 * g + j, G, stride=SX), :] = t[G * j : G * j + G]

        @pl.loop(0, 6)
        def _(g):
            tiles = [jnp.zeros((SX, 128), F32) for _ in range(3)]
            for b in range(8):
                off = 48 * b % 128
                at = 48 * b // 128
                v = s_ref[pl.ds(pl.multiple_of((8 * g + b) * SX, 8), SX), :]
                if off:
                    v = pltpu.roll(v, off, 1)
                if off + 48 > 128:
                    tiles[at] = tiles[at] + jnp.where(roll_lane >= off, v, 0.0)
                    tiles[at + 1] = tiles[at + 1] + jnp.where(roll_lane < off, v, 0.0)
                else:
                    tiles[at] = tiles[at] + v
            hi, lo = split(jnp.concatenate(tiles, axis=1))
            o = dot(mx, hi)
            o = o[:G] + o[G:] + dot(mx[:G], lo)
            for t in range(3):
                dest[pl.ds(3 * g + t, G, stride=18), :] = o[:, 128 * t : 128 * t + 128]

    @pl.loop(1, GX)
    def _(k):
        field(k, send.at[k])
        f_copy(k).start()

    field(0, recv.at[0])

    @pl.loop(1, GX)
    def _(k):
        f_copy(k).wait_recv()

    for s in range(SLOTS):
        anchor = (roots_s[0, 0, s] + HALO) % NX // BX
        k = ((my_y - anchor // 4 + 4) % 4) * 4 + (my_x - anchor % 4 + 4) % 4
        out[pl.ds(s, FLAT, stride=4), :] = recv[k]

    @pl.loop(1, GX)
    def _(k):
        f_copy(k).wait_send()
        root_copy(k).wait_send()

    own_d2d.wait_send()
    for i in range(4):
        x_copies[i].wait_send()
        x_relays[i].wait_send()
    for i in range(5):
        for d in range(2):
            z_all[i][d].wait_send()
            relays[i][d].wait_send()


def body(potential, frag_root):
    ytab, ztab, mx = tables()
    mx = jnp.asarray(mx)
    mx_hi, mx_lo = split(mx)
    mxt = jnp.concatenate([mx_hi, mx_lo], axis=0)
    root = jnp.pad(frag_root, ((0, 5), (0, 124)))
    vmem = pl.BlockSpec(memory_space=pltpu.VMEM)
    dma = pltpu.SemaphoreType.DMA
    out = pl.pallas_call(
        kernel,
        out_shape=jax.ShapeDtypeStruct((FLAT * SLOTS, 128), F32),
        in_specs=[pl.BlockSpec(memory_space=pl.ANY), vmem, vmem, vmem, vmem],
        out_specs=vmem,
        scratch_shapes=[
            pltpu.VMEM((GX, 8, 128), jnp.int32),
            pltpu.SMEM((GX, 8, 128), jnp.int32),
            pltpu.VMEM((EXT, YL, 128), F32),
            pltpu.VMEM((2, PACKS, 64, 128), F32),
            pltpu.VMEM((2, PACKS, YL, 128), F32),
            pltpu.VMEM((EXT, YL, 256), BF16),
            pltpu.VMEM((EXT, YL, 256), BF16),
            pltpu.VMEM((256, 256), BF16),
            pltpu.VMEM((2 * G, YL), BF16),
            pltpu.VMEM((G * SX, 128), F32),
            pltpu.VMEM((GX, FLAT, 128), F32),
            pltpu.VMEM((GX, FLAT, 128), F32),
            dma((GX,)), dma((GX,)), dma((1,)), dma((2,)),
            dma((4,)), dma((4,)), dma((4,)), dma((4,)),
            dma((5, 2)), dma((5, 2)), dma((5, 2)), dma((5, 2)),
            dma((GX,)), dma((GX,)),
        ],
        compiler_params=pltpu.CompilerParams(
            collective_id=0, has_side_effects=True, vmem_limit_bytes=66 * 1000 * 1000
        ),
    )(potential, root, jnp.asarray(ytab), jnp.asarray(ztab), mxt)
    return out.reshape(FLAT, SLOTS, 128).transpose(1, 0, 2).reshape(SLOTS, FLAT * 128)


def solution(mesh):
    return jax.shard_map(
        body,
        mesh=mesh,
        in_specs=(P("gx", "gy", "gz"), P(None, ("gx", "gy", "gz"))),
        out_specs=P(("gx", "gy", "gz"), None),
        check_vma=False,
    )
```

```python
import functools

import jax
import jax.numpy as jnp
import numpy as np
from jax import lax
from jax.experimental import pallas as pl
from jax.experimental.pallas import tpu as pltpu
from jax.sharding import PartitionSpec as P

MESH = pl.DeviceIdType.MESH
G = 48
BOX = 68
HALO = 34
BX = 60
BY = 60
BZ = 128
NX = 960
NY = 120
NZ = 512
GX = 16
SLOTS = 4
EXT = 128
YL = 128
FLAT = 864
SX = 72
ORDER = (6, 14, 9, 11, 10, 2, 8, 5, 15, 7, 13, 1, 3, 4, 12, 0)
RELAYED = ((6, 5, 1), (14, 15, 3), (9, 5, 4), (11, 15, 12))
FORWARD = (4, 5, 6, 7)
GROUP = 17
LEFT = 12
OWN = 19
PACKS = LEFT + OWN + LEFT
F32 = jnp.float32
BF16 = jnp.bfloat16


def interp_matrix():
    a = np.arange(G)[:, None]
    x = np.arange(BOX)[None, :]
    total = np.ones((G, BOX))
    for k in range(1, G // 2):
        total = total + 2.0 * np.cos(2.0 * np.pi * k * (a / G - x / BOX))
    return (total / BOX).astype(np.float32)


def tables():
    m = interp_matrix()
    ytab = np.zeros((248, 128), np.float32)
    for j in range(248):
        if j % NY < BOX:
            ytab[j, :G] = m[:, j % NY]
    ztab = np.zeros((512, 128), np.float32)
    for j in range(512):
        if j % 256 < BOX:
            ztab[j, :G] = m[:, j % 256]
    mx = np.zeros((G, SX), np.float32)
    mx[:, :BOX] = m
    return ytab, ztab, mx


def split(v):
    hi = v.astype(BF16)
    return hi, (v - hi.astype(F32)).astype(BF16)


def dot(a, b):
    return jnp.dot(a, b, preferred_element_type=F32)


def kernel(
    pot, root, ytab, ztab, mxt, out,
    roots, roots_s, xr, zsend, zrecv, e_ref, w_ref, my_ref, t1h, t1l, s_ref, fields, relay,
    root_send, root_recv, local_sem, own_sem, x_send, x_recv, xd_send, xd_recv,
    z_send, z_recv, zd_send, zd_recv, f_send, f_recv, r_send, r_recv,
):
    me = lax.axis_index("gx")
    core = lax.axis_index("gy")
    plane = lax.axis_index("gz")
    my_y, my_x = me // 4, me % 4

    def line(g):
        return {"gx": g, "gy": core, "gz": plane}

    def shifted(k):
        return ((my_y + k // 4) % 4) * 4 + (my_x + k % 4) % 4

    nxt, prv = (me + 1) % GX, (me + GX - 1) % GX
    partner = {"gx": me, "gy": 1 - core, "gz": plane}
    z_up = {"gx": me, "gy": core, "gz": (plane + 1) % 4}
    z_down = {"gx": me, "gy": core, "gz": (plane + 3) % 4}

    barrier = pltpu.get_barrier_semaphore()
    for d in (partner, z_up, z_down):
        pl.semaphore_signal(barrier, inc=1, device_id=d, device_id_type=MESH)

    @pl.loop(1, GX)
    def _(k):
        pl.semaphore_signal(barrier, inc=1, device_id=line(shifted(k)), device_id_type=MESH)

    pl.semaphore_wait(barrier, GX + 2)

    mine = pl.ds(pl.multiple_of(core * 64, 64), BY)
    mine64 = pl.ds(pl.multiple_of(core * 64, 64), 64)

    def remote(src, dst, ssem, rsem, to):
        return pltpu.make_async_remote_copy(
            src_ref=src, dst_ref=dst, send_sem=ssem, recv_sem=rsem, device_id=to, device_id_type=MESH
        )

    x_parts = ((26, 0, 18, nxt), (0, 94, 16, prv), (44, 18, 16, nxt), (16, 110, 18, prv))
    x_copies = [
        remote(pot.at[pl.ds(s, n)], xr.at[pl.ds(e, n), mine], x_send.at[i], x_recv.at[i], line(to))
        for i, (s, e, n, to) in enumerate(x_parts)
    ]
    def root_copy(k):
        return remote(root, roots.at[k], root_send.at[k], root_recv.at[k], line(shifted(k)))

    @pl.loop(1, GX)
    def _(k):
        root_copy(k).start()

    for c in x_copies:
        c.start()
    local = pltpu.make_async_copy(pot, xr.at[pl.ds(HALO, BX), mine], local_sem.at[0])
    local.start()
    own_d2d = remote(pot, xr.at[pl.ds(HALO, BX), mine], own_sem.at[0], own_sem.at[1], partner)
    own_d2d.start()
    roots[0] = root[...]

    local.wait()
    own_d2d.wait_recv()

    @pl.loop(0, EXT)
    def _(x):
        xr[x, 60:64, :] = jnp.zeros((4, 128), F32)
        xr[x, 124:128, :] = jnp.zeros((4, 128), F32)

    lane = lax.broadcasted_iota(jnp.int32, (64, 128), 1)

    def pack(first, count, slab):
        @pl.loop(0, count)
        def _(p):
            x = slab + 3 * p
            up = jnp.zeros((64, 128), F32)
            down = jnp.zeros((64, 128), F32)
            for j in range(3):
                v = xr[x + j, mine64, :]
                low = 94 - 34 * j
                up = jnp.where((lane >= low) & (lane < low + 34), pltpu.roll(v, (128 - 34 * j) % 128, 1), up)
                down = jnp.where((lane >= 34 * j) & (lane < 34 * j + 34), pltpu.roll(v, 34 * j, 1), down)
            zsend[0, first + p] = up
            zsend[1, first + p] = down

    def z_copies(i, first, count):
        rows = pl.ds(first, count)
        return [
            remote(zsend.at[d, rows], zrecv.at[d, rows, mine64], z_send.at[i, d], z_recv.at[i, d], to)
            for d, to in enumerate((z_up, z_down))
        ]

    def z_relays(i, first, count):
        rows = pl.ds(first, count)
        return [
            remote(zrecv.at[d, rows, mine64], zrecv.at[d, rows, mine64], zd_send.at[i, d], zd_recv.at[i, d], partner)
            for d in range(2)
        ]

    def x_relay(i):
        _, e, n, _ = x_parts[i]
        return remote(xr.at[pl.ds(e, n), mine], xr.at[pl.ds(e, n), mine], xd_send.at[i], xd_recv.at[i], partner)

    lane_y = lax.broadcasted_iota(jnp.int32, (YL, 128), 1)

    def convert(first, count, slab):
        @pl.loop(0, count)
        def _(p):
            below = zrecv[0, first + p]
            above = zrecv[1, first + p]
            for j in range(3):
                x = slab + 3 * p + j
                v = xr[x]
                h, l = split(v)
                e_ref[x, 0:128, 0:128] = h
                e_ref[x, 128:256, 0:128] = l
                edge = jnp.where(
                    lane_y < 34,
                    pltpu.roll(above, (128 - 34 * j) % 128, 1),
                    jnp.where(lane_y >= 94, pltpu.roll(below, 34 * j, 1), 0.0),
                )
                h, l = split(edge)
                e_ref[x, 0:128, 128:256] = h
                e_ref[x, 128:256, 128:256] = l

    z_parts = ((0, OWN, 36), (OWN, 6, 0), (OWN + 6, 6, 92), (OWN + 12, 6, 18), (OWN + 18, 6, 110))
    z_all = [z_copies(i, f, n) for i, (f, n, _) in enumerate(z_parts)]
    relays = [z_relays(i, f, n) for i, (f, n, _) in enumerate(z_parts)]
    x_relays = [x_relay(i) for i in range(4)]

    def z_arrived(i):
        for d in range(2):
            z_all[i][d].wait_recv()
            relays[i][d].start()

    pack(*z_parts[0])
    for c in z_all[0]:
        c.start()
    for i in range(4):
        x_copies[i].wait_recv()
        x_relays[i].start()
        pack(*z_parts[i + 1])
        for c in z_all[i + 1]:
            c.start()
        if i == 2:
            z_arrived(0)
    @pl.loop(1, GX)
    def _(k):
        root_copy(k).wait_recv()

    pltpu.sync_copy(roots, roots_s)
    s_ref[...] = jnp.zeros(s_ref.shape, F32)
    for i in range(4):
        x_relays[i].wait_recv()
    for i in range(5):
        if i:
            z_arrived(i)
        if i >= 1:
            for d in range(2):
                relays[i - 1][d].wait_recv()
            convert(*z_parts[i - 1])
    for d in range(2):
        relays[4][d].wait_recv()
    convert(*z_parts[4])

    mx = mxt[...]
    roll_lane = lax.broadcasted_iota(jnp.int32, (SX, 128), 1)
    relay_legs = {k: leg for k, leg, _ in RELAYED}

    def f_copy(i):
        k = ORDER[i]
        if k in relay_legs:
            j = [r[0] for r in RELAYED].index(k)
            return remote(fields.at[i], relay.at[j], f_send.at[i], r_recv.at[j], line(shifted(relay_legs[k])))
        return remote(fields.at[i], fields.at[GX + i], f_send.at[i], f_recv.at[i], line(shifted(k)))

    def forward(j):
        k, _, leg = RELAYED[j]
        i = ORDER.index(k)
        return remote(relay.at[j], fields.at[GX + i], r_send.at[j], f_recv.at[i], line(shifted(leg)))

    def arrival(i):
        return remote(fields.at[i], fields.at[GX + i], f_send.at[i], f_recv.at[i], line(shifted(1)))

    def choose(i, values):
        total = jnp.int32(0)
        for c, v in enumerate(values):
            total = jnp.where(i == c, v, total)
        return total

    def field(i):
        k = choose(i, ORDER)
        back = ((4 - k // 4) % 4) * 4 + (4 - k % 4) % 4
        rx, ry, rz = jnp.int32(0), jnp.int32(0), jnp.int32(0)
        for s in range(SLOTS):
            fx = roots_s[back, 0, s]
            mine_too = (fx + HALO) % NX // BX == me
            rx = jnp.where(mine_too, fx, rx)
            ry = jnp.where(mine_too, roots_s[back, 1, s], ry)
            rz = jnp.where(mine_too, roots_s[back, 2, s], rz)
        sx = jnp.minimum((rx + HALO - me * BX + NX) % NX, BX - 1)
        sy = ry
        sz = (rz - plane * BZ + NZ) % 256
        my_t = jnp.concatenate([ytab[pl.ds(NY - sy, 64), :], ytab[pl.ds(NY + BY - sy, 64), :]], axis=0)
        my_hi, my_lo = split(my_t.T[0:G, :])
        my_ref[0:G, 0:128] = my_hi
        my_ref[0:G, 128:256] = my_hi
        my_ref[G : 2 * G, 0:128] = my_lo
        my_ref[G : 2 * G, 128:256] = my_lo
        z_hi, z_lo = split(ztab[pl.ds(256 - sz, 256), :])
        w_ref[:, 0:128] = z_hi
        w_ref[:, 128:256] = z_lo

        @pl.loop(0, BOX // GROUP)
        def _(g):
            both = my_ref[...]
            for j in range(GROUP):
                t = dot(both, e_ref[sx + GROUP * g + j])
                hi, lo = split(t[:G] + t[G:])
                rows = pl.ds(pl.multiple_of((GROUP * g + j) * G, G), G)
                t1h[rows, :] = hi
                t1l[rows, :] = lo

        @pl.loop(0, BOX // GROUP)
        def _(g):
            rows = pl.ds(pl.multiple_of(GROUP * g * G, G), GROUP * G)
            q = dot(t1h[rows, :], w_ref[...])
            t = q[:, :128] + q[:, 128:] + dot(t1l[rows, :], w_ref[:, 0:128])
            for j in range(GROUP):
                s_ref[pl.ds(GROUP * g + j, G, stride=SX), :] = t[G * j : G * j + G]

        for g in range(6):
            tiles = [jnp.zeros((SX, 128), F32) for _ in range(3)]
            for b in range(8):
                off = 48 * b % 128
                at = 48 * b // 128
                v = s_ref[pl.ds((8 * g + b) * SX, SX), :]
                if off:
                    v = pltpu.roll(v, off, 1)
                if off + 48 > 128:
                    tiles[at] = tiles[at] + jnp.where(roll_lane >= off, v, 0.0)
                    tiles[at + 1] = tiles[at + 1] + jnp.where(roll_lane < off, v, 0.0)
                else:
                    tiles[at] = tiles[at] + v
            r = jnp.concatenate([jnp.concatenate(tiles, axis=1), jnp.zeros((8, 384), F32)], axis=0)
            hi, lo = split(r)
            o = dot(mx, jnp.concatenate([hi, lo], axis=0))
            o = o[:G] + o[G:]
            for t in range(3):
                fields[i, pl.ds(3 * g + t, G, stride=18), :] = o[:, 128 * t : 128 * t + 128]

    @pl.loop(0, GX)
    def _(i):
        field(i)
        for c in range(GX - 1):

            @pl.when(i == c)
            def _():
                f_copy(c).start()
                for j, at in enumerate(FORWARD):
                    if at == c:
                        f_copy(ORDER.index(RELAYED[j][0])).wait_recv()
                        forward(j).start()

    for i in range(GX - 1):
        arrival(i).wait_recv()

    for s in range(SLOTS):
        anchor = (roots_s[0, 0, s] + HALO) % NX // BX
        k = ((my_y - anchor // 4 + 4) % 4) * 4 + (my_x - anchor % 4 + 4) % 4
        at = choose(k, [GX + ORDER.index(c) if c else ORDER.index(0) for c in range(GX)])
        out[pl.ds(s, FLAT, stride=4), :] = fields[at]

    for i in range(GX - 1):
        f_copy(i).wait_send()
    for j in range(len(RELAYED)):
        forward(j).wait_send()

    @pl.loop(1, GX)
    def _(k):
        root_copy(k).wait_send()

    own_d2d.wait_send()
    for i in range(4):
        x_copies[i].wait_send()
        x_relays[i].wait_send()
    for i in range(5):
        for d in range(2):
            z_all[i][d].wait_send()
            relays[i][d].wait_send()


def body(potential, frag_root):
    ytab, ztab, mx = tables()
    mx = jnp.asarray(mx)
    mx_hi, mx_lo = split(mx)
    zero = jnp.zeros((G, 8), BF16)
    mxt = jnp.concatenate(
        [jnp.concatenate([m, zero, m, zero], axis=1) for m in (mx_hi, mx_lo)], axis=0
    )
    root = jnp.pad(frag_root, ((0, 5), (0, 124)))
    vmem = pl.BlockSpec(memory_space=pltpu.VMEM)
    dma = pltpu.SemaphoreType.DMA
    out = pl.pallas_call(
        kernel,
        out_shape=jax.ShapeDtypeStruct((FLAT * SLOTS, 128), F32),
        in_specs=[pl.BlockSpec(memory_space=pl.ANY), vmem, vmem, vmem, vmem],
        out_specs=vmem,
        scratch_shapes=[
            pltpu.VMEM((GX, 8, 128), jnp.int32),
            pltpu.SMEM((GX, 8, 128), jnp.int32),
            pltpu.VMEM((EXT, YL, 128), F32),
            pltpu.VMEM((2, PACKS, 64, 128), F32),
            pltpu.VMEM((2, PACKS, YL, 128), F32),
            pltpu.VMEM((EXT, 2 * YL, 256), BF16),
            pltpu.VMEM((256, 256), BF16),
            pltpu.VMEM((2 * G, 2 * YL), BF16),
            pltpu.VMEM((BOX * G, 256), BF16),
            pltpu.VMEM((BOX * G, 256), BF16),
            pltpu.VMEM((G * SX, 128), F32),
            pltpu.VMEM((2 * GX, FLAT, 128), F32),
            pltpu.VMEM((len(RELAYED), FLAT, 128), F32),
            dma((GX,)), dma((GX,)), dma((1,)), dma((2,)),
            dma((4,)), dma((4,)), dma((4,)), dma((4,)),
            dma((5, 2)), dma((5, 2)), dma((5, 2)), dma((5, 2)),
            dma((GX,)), dma((GX,)), dma((4,)), dma((4,)),
        ],
        compiler_params=pltpu.CompilerParams(
            collective_id=0, has_side_effects=True, vmem_limit_bytes=66 * 1000 * 1000
        ),
    )(potential, root, jnp.asarray(ytab), jnp.asarray(ztab), mxt)
    return out.reshape(FLAT, SLOTS, 128).transpose(1, 0, 2).reshape(SLOTS, FLAT * 128)


def solution(mesh):
    return jax.shard_map(
        body,
        mesh=mesh,
        in_specs=(P("gx", "gy", "gz"), P(None, ("gx", "gy", "gz"))),
        out_specs=P(("gx", "gy", "gz"), None),
        check_vma=False,
    )
```

```python
import functools

import jax
import jax.numpy as jnp
import numpy as np
from jax import lax
from jax.experimental import pallas as pl
from jax.experimental.pallas import tpu as pltpu
from jax.sharding import PartitionSpec as P

MESH = pl.DeviceIdType.MESH
G = 48
BOX = 68
HALO = 34
BX = 60
BY = 60
BZ = 128
NX = 960
NY = 120
NZ = 512
GX = 16
SLOTS = 4
EXT = 128
YL = 128
FLAT = 864
SX = 72
ORDER = (6, 14, 9, 11, 10, 2, 8, 5, 15, 7, 13, 1, 3, 4, 12, 0)
RELAYED = ((6, 5, 1), (14, 15, 3), (9, 5, 4), (11, 15, 12))
FORWARD = (4, 5, 6, 7)
GROUP = 17
LEFT = 12
OWN = 19
PACKS = LEFT + OWN + LEFT
F32 = jnp.float32
BF16 = jnp.bfloat16


def interp_matrix():
    a = np.arange(G)[:, None]
    x = np.arange(BOX)[None, :]
    total = np.ones((G, BOX))
    for k in range(1, G // 2):
        total = total + 2.0 * np.cos(2.0 * np.pi * k * (a / G - x / BOX))
    return (total / BOX).astype(np.float32)


def tables():
    m = interp_matrix()
    ytab = np.zeros((248, 128), np.float32)
    for j in range(248):
        if j % NY < BOX:
            ytab[j, :G] = m[:, j % NY]
    ztab = np.zeros((512, 128), np.float32)
    for j in range(512):
        if j % 256 < BOX:
            ztab[j, :G] = m[:, j % 256]
    mx = np.zeros((G, SX), np.float32)
    mx[:, :BOX] = m
    return ytab, ztab, mx


def split(v):
    hi = v.astype(BF16)
    return hi, (v - hi.astype(F32)).astype(BF16)


def dot(a, b):
    return jnp.dot(a, b, preferred_element_type=F32)


def kernel(
    pot, root, ytab, ztab, mxt, out,
    roots, roots_s, xr, zsend, zrecv, e_ref, w_ref, my_ref, t1h, t1l, s_ref, fields, relay,
    ready, root_send, root_recv, local_sem, own_sem, x_send, x_recv, xd_send, xd_recv,
    z_send, z_recv, zd_send, zd_recv, f_send, f_recv, r_send, r_recv,
):
    me = lax.axis_index("gx")
    core = lax.axis_index("gy")
    plane = lax.axis_index("gz")
    my_y, my_x = me // 4, me % 4

    def line(g):
        return {"gx": g, "gy": core, "gz": plane}

    def shifted(k):
        return ((my_y + k // 4) % 4) * 4 + (my_x + k % 4) % 4

    nxt, prv = (me + 1) % GX, (me + GX - 1) % GX
    partner = {"gx": me, "gy": 1 - core, "gz": plane}
    z_up = {"gx": me, "gy": core, "gz": (plane + 1) % 4}
    z_down = {"gx": me, "gy": core, "gz": (plane + 3) % 4}

    barrier = pltpu.get_barrier_semaphore()
    first = [partner, z_up, z_down, line(nxt), line(prv)] + [line(shifted(k)) for k in (1, 2, 3, 4, 8, 12)]
    for d in first:
        pl.semaphore_signal(barrier, inc=1, device_id=d, device_id_type=MESH)
    pl.semaphore_wait(barrier, len(first))
    for k in (4, 8, 12):
        pl.semaphore_signal(ready, inc=1, device_id=line(shifted(k)), device_id_type=MESH)

    mine = pl.ds(pl.multiple_of(core * 64, 64), BY)
    mine64 = pl.ds(pl.multiple_of(core * 64, 64), 64)

    def remote(src, dst, ssem, rsem, to):
        return pltpu.make_async_remote_copy(
            src_ref=src, dst_ref=dst, send_sem=ssem, recv_sem=rsem, device_id=to, device_id_type=MESH
        )

    x_parts = (
        (26, 0, 18, nxt), (0, 94, 16, prv), (44, 18, 9, nxt), (16, 110, 9, prv), (53, 27, 7, nxt), (25, 119, 9, prv)
    )
    x_copies = [
        remote(pot.at[pl.ds(s, n)], xr.at[pl.ds(e, n), mine], x_send.at[i], x_recv.at[i], line(to))
        for i, (s, e, n, to) in enumerate(x_parts)
    ]
    def root_copy(k):
        return remote(root, roots.at[k], root_send.at[k], root_recv.at[k], line(shifted(k)))

    for c in x_copies:
        c.start()
    local = pltpu.make_async_copy(pot, xr.at[pl.ds(HALO, BX), mine], local_sem.at[0])
    local.start()
    own_d2d = remote(pot, xr.at[pl.ds(HALO, BX), mine], own_sem.at[0], own_sem.at[1], partner)
    own_d2d.start()
    roots[0] = root[...]
    s_ref[...] = jnp.zeros(s_ref.shape, F32)
    local.wait()

    lane = lax.broadcasted_iota(jnp.int32, (64, 128), 1)

    def pack(first, count, slab):
        @pl.loop(0, count)
        def _(p):
            x = slab + 3 * p
            up = jnp.zeros((64, 128), F32)
            down = jnp.zeros((64, 128), F32)
            for j in range(3):
                v = xr[x + j, mine64, :]
                low = 94 - 34 * j
                up = jnp.where((lane >= low) & (lane < low + 34), pltpu.roll(v, (128 - 34 * j) % 128, 1), up)
                down = jnp.where((lane >= 34 * j) & (lane < 34 * j + 34), pltpu.roll(v, 34 * j, 1), down)
            zsend[0, first + p] = up
            zsend[1, first + p] = down

    def z_copies(i, first, count):
        rows = pl.ds(first, count)
        return [
            remote(zsend.at[d, rows, 0:BY], zrecv.at[d, rows, mine], z_send.at[i, d], z_recv.at[i, d], to)
            for d, to in enumerate((z_up, z_down))
        ]

    def z_relays(i, first, count):
        rows = pl.ds(first, count)
        return [
            remote(zrecv.at[d, rows, mine], zrecv.at[d, rows, mine], zd_send.at[i, d], zd_recv.at[i, d], partner)
            for d in range(2)
        ]

    def x_relay(i):
        _, e, n, _ = x_parts[i]
        return remote(xr.at[pl.ds(e, n), mine], xr.at[pl.ds(e, n), mine], xd_send.at[i], xd_recv.at[i], partner)

    lane_y = lax.broadcasted_iota(jnp.int32, (YL, 128), 1)
    real = lax.broadcasted_iota(jnp.int32, (YL, 128), 0) % 64 < BY

    def convert(first, count, slab):
        @pl.loop(0, count)
        def _(p):
            below = zrecv[0, first + p]
            above = zrecv[1, first + p]
            for j in range(3):
                x = slab + 3 * p + j
                v = jnp.where(real, xr[x], 0.0)
                h, l = split(v)
                e_ref[x, 0:128, 0:128] = h
                e_ref[x, 128:256, 0:128] = l
                edge = jnp.where(
                    real & (lane_y < 34),
                    pltpu.roll(above, (128 - 34 * j) % 128, 1),
                    jnp.where(real & (lane_y >= 94), pltpu.roll(below, 34 * j, 1), 0.0),
                )
                h, l = split(edge)
                e_ref[x, 0:128, 128:256] = h
                e_ref[x, 128:256, 128:256] = l

    z_parts = ((0, OWN, 36), (19, 6, 0), (25, 6, 92), (31, 3, 18), (34, 3, 110), (37, 3, 27), (40, 3, 119))
    z_all = [z_copies(i, f, n) for i, (f, n, _) in enumerate(z_parts)]
    relays = [z_relays(i, f, n) for i, (f, n, _) in enumerate(z_parts)]
    x_relays = [x_relay(i) for i in range(6)]

    def x_arrived(i):
        x_copies[i].wait_recv()
        x_relays[i].start()
        pack(*z_parts[i + 1])
        for c in z_all[i + 1]:
            c.start()

    def z_arrived(i):
        for d in range(2):
            z_all[i][d].wait_recv()
            relays[i][d].start()

    def complete(i):
        if i:
            x_relays[i - 1].wait_recv()
        for d in range(2):
            relays[i][d].wait_recv()
        convert(*z_parts[i])

    pack(*z_parts[0])
    for c in z_all[0]:
        c.start()
    pl.semaphore_wait(ready, 3)

    @pl.loop(1, GX)
    def _(k):
        root_copy(k).start()

    x_arrived(0)
    x_arrived(1)
    z_arrived(0)

    @pl.loop(1, GX)
    def _(k):
        root_copy(k).wait_recv()

    pltpu.sync_copy(roots, roots_s)
    own_d2d.wait_recv()
    complete(0)
    x_arrived(2)
    x_arrived(3)
    z_arrived(1)
    z_arrived(2)
    x_arrived(4)
    x_arrived(5)
    complete(1)
    complete(2)
    z_arrived(3)
    z_arrived(4)
    complete(3)
    complete(4)
    z_arrived(5)
    z_arrived(6)
    complete(5)
    complete(6)

    mx = mxt[...]
    roll_lane = lax.broadcasted_iota(jnp.int32, (SX, 128), 1)
    relay_legs = {k: leg for k, leg, _ in RELAYED}

    def f_copy(i):
        k = ORDER[i]
        if k in relay_legs:
            j = [r[0] for r in RELAYED].index(k)
            return remote(fields.at[i], relay.at[j], f_send.at[i], r_recv.at[j], line(shifted(relay_legs[k])))
        return remote(fields.at[i], fields.at[GX + i], f_send.at[i], f_recv.at[i], line(shifted(k)))

    def forward(j):
        k, _, leg = RELAYED[j]
        i = ORDER.index(k)
        return remote(relay.at[j], fields.at[GX + i], r_send.at[j], f_recv.at[i], line(shifted(leg)))

    def arrival(i):
        return remote(fields.at[i], fields.at[GX + i], f_send.at[i], f_recv.at[i], line(shifted(1)))

    def choose(i, values):
        total = jnp.int32(0)
        for c, v in enumerate(values):
            total = jnp.where(i == c, v, total)
        return total

    def field(i):
        k = choose(i, ORDER)
        back = ((4 - k // 4) % 4) * 4 + (4 - k % 4) % 4
        rx, ry, rz = jnp.int32(0), jnp.int32(0), jnp.int32(0)
        for s in range(SLOTS):
            fx = roots_s[back, 0, s]
            mine_too = (fx + HALO) % NX // BX == me
            rx = jnp.where(mine_too, fx, rx)
            ry = jnp.where(mine_too, roots_s[back, 1, s], ry)
            rz = jnp.where(mine_too, roots_s[back, 2, s], rz)
        sx = jnp.minimum((rx + HALO - me * BX + NX) % NX, BX - 1)
        sy = ry
        sz = (rz - plane * BZ + NZ) % 256
        my_t = jnp.concatenate([ytab[pl.ds(NY - sy, 64), :], ytab[pl.ds(NY + BY - sy, 64), :]], axis=0)
        my_hi, my_lo = split(my_t.T[0:G, :])
        my_ref[0:G, 0:128] = my_hi
        my_ref[0:G, 128:256] = my_hi
        my_ref[G : 2 * G, 0:128] = my_lo
        my_ref[G : 2 * G, 128:256] = my_lo
        z_hi, z_lo = split(ztab[pl.ds(256 - sz, 256), :])
        w_ref[:, 0:128] = z_hi
        w_ref[:, 128:256] = z_lo

        both = my_ref[...]
        for g in range(BOX // GROUP):
            for j in range(GROUP):
                t = dot(both, e_ref[sx + GROUP * g + j])
                hi, lo = split(t[:G] + t[G:])
                rows = pl.ds((GROUP * g + j) * G, G)
                t1h[rows, :] = hi
                t1l[rows, :] = lo
            rows = pl.ds(GROUP * g * G, GROUP * G)
            q = dot(t1h[rows, :], w_ref[...])
            t = q[:, :128] + q[:, 128:] + dot(t1l[rows, :], w_ref[:, 0:128])
            for j in range(GROUP):
                s_ref[pl.ds(GROUP * g + j, G, stride=SX), :] = t[G * j : G * j + G]

        for g in range(6):
            tiles = [jnp.zeros((SX, 128), F32) for _ in range(3)]
            for b in range(8):
                off = 48 * b % 128
                at = 48 * b // 128
                v = s_ref[pl.ds((8 * g + b) * SX, SX), :]
                if off:
                    v = pltpu.roll(v, off, 1)
                if off + 48 > 128:
                    tiles[at] = tiles[at] + jnp.where(roll_lane >= off, v, 0.0)
                    tiles[at + 1] = tiles[at + 1] + jnp.where(roll_lane < off, v, 0.0)
                else:
                    tiles[at] = tiles[at] + v
            r = jnp.concatenate([jnp.concatenate(tiles, axis=1), jnp.zeros((8, 384), F32)], axis=0)
            hi, lo = split(r)
            o = dot(mx, jnp.concatenate([hi, lo], axis=0))
            o = o[:G] + o[G:]
            for t in range(3):
                fields[i, pl.ds(3 * g + t, G, stride=18), :] = o[:, 128 * t : 128 * t + 128]

    @pl.loop(0, GX)
    def _(i):
        field(i)
        for c in range(GX - 1):

            @pl.when(i == c)
            def _():
                f_copy(c).start()
                for j, at in enumerate(FORWARD):
                    if at == c:
                        f_copy(ORDER.index(RELAYED[j][0])).wait_recv()
                        forward(j).start()

    for i in range(GX - 1):
        arrival(i).wait_recv()

    for s in range(SLOTS):
        anchor = (roots_s[0, 0, s] + HALO) % NX // BX
        k = ((my_y - anchor // 4 + 4) % 4) * 4 + (my_x - anchor % 4 + 4) % 4
        at = choose(k, [GX + ORDER.index(c) if c else ORDER.index(0) for c in range(GX)])
        out[pl.ds(s, FLAT, stride=4), :] = fields[at]

    for i in range(GX - 1):
        f_copy(i).wait_send()
    for j in range(len(RELAYED)):
        forward(j).wait_send()

    @pl.loop(1, GX)
    def _(k):
        root_copy(k).wait_send()

    own_d2d.wait_send()
    for i in range(6):
        x_copies[i].wait_send()
        x_relays[i].wait_send()
    for i in range(7):
        for d in range(2):
            z_all[i][d].wait_send()
            relays[i][d].wait_send()


def body(potential, frag_root):
    ytab, ztab, mx = tables()
    mx = jnp.asarray(mx)
    mx_hi, mx_lo = split(mx)
    zero = jnp.zeros((G, 8), BF16)
    mxt = jnp.concatenate(
        [jnp.concatenate([m, zero, m, zero], axis=1) for m in (mx_hi, mx_lo)], axis=0
    )
    vmem = pl.BlockSpec(memory_space=pltpu.VMEM)
    dma = pltpu.SemaphoreType.DMA
    out = pl.pallas_call(
        kernel,
        out_shape=jax.ShapeDtypeStruct((FLAT * SLOTS, 128), F32),
        in_specs=[pl.BlockSpec(memory_space=pl.ANY), vmem, vmem, vmem, vmem],
        out_specs=vmem,
        scratch_shapes=[
            pltpu.VMEM((GX, 3, SLOTS), jnp.int32),
            pltpu.SMEM((GX, 3, SLOTS), jnp.int32),
            pltpu.VMEM((EXT, YL, 128), F32),
            pltpu.VMEM((2, PACKS, 64, 128), F32),
            pltpu.VMEM((2, PACKS, YL, 128), F32),
            pltpu.VMEM((EXT, 2 * YL, 256), BF16),
            pltpu.VMEM((256, 256), BF16),
            pltpu.VMEM((2 * G, 2 * YL), BF16),
            pltpu.VMEM((BOX * G, 256), BF16),
            pltpu.VMEM((BOX * G, 256), BF16),
            pltpu.VMEM((G * SX, 128), F32),
            pltpu.VMEM((2 * GX, FLAT, 128), F32),
            pltpu.VMEM((len(RELAYED), FLAT, 128), F32),
            pltpu.SemaphoreType.REGULAR, dma((GX,)), dma((GX,)), dma((1,)), dma((2,)),
            dma((6,)), dma((6,)), dma((6,)), dma((6,)),
            dma((7, 2)), dma((7, 2)), dma((7, 2)), dma((7, 2)),
            dma((GX,)), dma((GX,)), dma((4,)), dma((4,)),
        ],
        compiler_params=pltpu.CompilerParams(
            collective_id=0, has_side_effects=True, vmem_limit_bytes=66 * 1000 * 1000
        ),
    )(potential, frag_root, jnp.asarray(ytab), jnp.asarray(ztab), mxt)
    return out.reshape(FLAT, SLOTS, 128).transpose(1, 0, 2).reshape(SLOTS, FLAT * 128)


def solution(mesh):
    return jax.shard_map(
        body,
        mesh=mesh,
        in_specs=(P("gx", "gy", "gz"), P(None, ("gx", "gy", "gz"))),
        out_specs=P(("gx", "gy", "gz"), None),
        check_vma=False,
    )
```

```python
import functools

import jax
import jax.numpy as jnp
import numpy as np
from jax import lax
from jax.experimental import pallas as pl
from jax.experimental.pallas import tpu as pltpu
from jax.sharding import PartitionSpec as P

MESH = pl.DeviceIdType.MESH
G = 48
BOX = 68
HALO = 34
BX = 60
BY = 60
BZ = 128
NX = 960
NY = 120
NZ = 512
GX = 16
SLOTS = 4
EXT = 128
YL = 128
FLAT = 864
SX = 72
ORDER = (6, 14, 9, 11, 10, 2, 8, 5, 15, 7, 13, 1, 3, 4, 12, 0)
RELAYED = ((6, 5, 1), (14, 15, 3), (9, 5, 4), (11, 15, 12))
FORWARD = (4, 5, 6, 7)
GROUP = 17
UNITS = 19
OFFSETS = (0, 34, 68, 102, 8, 42, 76)
F32 = jnp.float32
BF16 = jnp.bfloat16


def interp_matrix():
    a = np.arange(G)[:, None]
    x = np.arange(BOX)[None, :]
    total = np.ones((G, BOX))
    for k in range(1, G // 2):
        total = total + 2.0 * np.cos(2.0 * np.pi * k * (a / G - x / BOX))
    return (total / BOX).astype(np.float32)


def tables():
    m = interp_matrix()
    ytab = np.zeros((248, 128), np.float32)
    for j in range(248):
        if j % NY < BOX:
            ytab[j, :G] = m[:, j % NY]
    ztab = np.zeros((512, 128), np.float32)
    for j in range(512):
        if j % 256 < BOX:
            ztab[j, :G] = m[:, j % 256]
    mx = np.zeros((G, SX), np.float32)
    mx[:, :BOX] = m
    return ytab, ztab, mx


def split(v):
    hi = v.astype(BF16)
    return hi, (v - hi.astype(F32)).astype(BF16)


def dot(a, b):
    return jnp.dot(a, b, preferred_element_type=F32)


def kernel(
    pot, root, ytab, ztab, mxt, out,
    roots, roots_s, xr, zsend, zrecv, e_ref, w_ref, my_ref, t1h, t1l, s_ref, fields, relay,
    ready, root_send, root_recv, local_sem, own_sem, x_send, x_recv, xd_send, xd_recv,
    z_send, z_recv, zd_send, zd_recv, f_send, f_recv, r_send, r_recv,
):
    me = lax.axis_index("gx")
    core = lax.axis_index("gy")
    plane = lax.axis_index("gz")
    my_y, my_x = me // 4, me % 4

    def line(g):
        return {"gx": g, "gy": core, "gz": plane}

    def shifted(k):
        return ((my_y + k // 4) % 4) * 4 + (my_x + k % 4) % 4

    nxt, prv = (me + 1) % GX, (me + GX - 1) % GX
    partner = {"gx": me, "gy": 1 - core, "gz": plane}
    z_up = {"gx": me, "gy": core, "gz": (plane + 1) % 4}
    z_down = {"gx": me, "gy": core, "gz": (plane + 3) % 4}

    barrier = pltpu.get_barrier_semaphore()
    first = [partner, z_up, z_down, line(nxt), line(prv)] + [line(shifted(k)) for k in (1, 2, 3, 4, 8, 12)]
    for d in first:
        pl.semaphore_signal(barrier, inc=1, device_id=d, device_id_type=MESH)
    pl.semaphore_wait(barrier, len(first))
    for k in (4, 8, 12):
        pl.semaphore_signal(ready, inc=1, device_id=line(shifted(k)), device_id_type=MESH)

    mine = pl.ds(pl.multiple_of(core * 64, 64), BY)
    mine64 = pl.ds(pl.multiple_of(core * 64, 64), 64)

    def remote(src, dst, ssem, rsem, to):
        return pltpu.make_async_remote_copy(
            src_ref=src, dst_ref=dst, send_sem=ssem, recv_sem=rsem, device_id=to, device_id_type=MESH
        )

    x_parts = (
        (26, 0, 14, nxt), (0, 94, 13, prv), (40, 14, 14, nxt), (13, 107, 14, prv), (54, 28, 6, nxt), (27, 121, 7, prv)
    )
    x_copies = [
        remote(pot.at[pl.ds(s, n)], xr.at[pl.ds(e, n), mine], x_send.at[i], x_recv.at[i], line(to))
        for i, (s, e, n, to) in enumerate(x_parts)
    ]
    def root_copy(k):
        return remote(root, roots.at[k], root_send.at[k], root_recv.at[k], line(shifted(k)))

    for c in x_copies:
        c.start()
    local = pltpu.make_async_copy(pot, xr.at[pl.ds(HALO, BX), mine], local_sem.at[0])
    local.start()
    own_d2d = remote(pot, xr.at[pl.ds(HALO, BX), mine], own_sem.at[0], own_sem.at[1], partner)
    own_d2d.start()
    roots[0] = root[...]
    local.wait()

    lane = lax.broadcasted_iota(jnp.int32, (64, 128), 1)

    def pack(first, count, slab):
        @pl.loop(0, count)
        def _(u):
            tiles = [[jnp.zeros((64, 128), F32) for _ in range(2)] for _ in range(2)]
            for j, off in enumerate(OFFSETS):
                v = xr[slab + 7 * u + j, mine64, :]
                for d, at in enumerate((off - 94, off)):
                    w = pltpu.roll(v, at % 128, 1) if at % 128 else v
                    if j == 3:
                        tiles[d][0] = jnp.where(lane >= off, w, tiles[d][0])
                        tiles[d][1] = jnp.where(lane < off + 34 - 128, w, tiles[d][1])
                    else:
                        inside = (lane >= off) & (lane < off + 34)
                        tiles[d][j // 4] = jnp.where(inside, w, tiles[d][j // 4])
            for d in range(2):
                for t in range(2):
                    zsend[d, 2 * (first + u) + t] = tiles[d][t]

    def z_copies(i, first, count):
        rows = pl.ds(2 * first, 2 * count)
        return [
            remote(zsend.at[d, rows, 0:BY], zrecv.at[d, rows, mine], z_send.at[i, d], z_recv.at[i, d], to)
            for d, to in enumerate((z_up, z_down))
        ]

    def z_relays(i, first, count):
        rows = pl.ds(2 * first, 2 * count)
        return [
            remote(zrecv.at[d, rows, mine], zrecv.at[d, rows, mine], zd_send.at[i, d], zd_recv.at[i, d], partner)
            for d in range(2)
        ]

    def x_relay(i):
        _, e, n, _ = x_parts[i]
        return remote(xr.at[pl.ds(e, n), mine], xr.at[pl.ds(e, n), mine], xd_send.at[i], xd_recv.at[i], partner)

    lane_y = lax.broadcasted_iota(jnp.int32, (YL, 128), 1)
    def convert_own(slab, count):
        @pl.loop(0, count // 2)
        def _(p):
            for j in range(2):
                x = slab + 2 * p + j
                h, l = split(xr[x])
                e_ref[x, 0:128, 0:128] = h
                e_ref[x, 128:256, 0:128] = l

    def convert_edges(first, count, slab):
        @pl.loop(0, count)
        def _(u):
            below = [zrecv[0, 2 * (first + u) + t] for t in range(2)]
            above = [zrecv[1, 2 * (first + u) + t] for t in range(2)]
            for j, off in enumerate(OFFSETS):
                x = slab + 7 * u + j
                parts = []
                for tiles, at in ((above, -off), (below, 94 - off)):
                    v = jnp.where(lane_y >= off, tiles[0], tiles[1]) if j == 3 else tiles[j // 4]
                    parts.append(pltpu.roll(v, at % 128, 1) if at % 128 else v)
                h, l = split(jnp.where(lane_y < 34, parts[0], jnp.where(lane_y >= 94, parts[1], 0.0)))
                e_ref[x, 0:128, 128:256] = h
                e_ref[x, 128:256, 128:256] = l

    z_parts = ((0, 9, 35), (9, 2, 0), (11, 2, 93), (13, 2, 14), (15, 2, 107), (17, 1, 28), (18, 1, 121))
    z_all = [z_copies(i, f, n) for i, (f, n, _) in enumerate(z_parts)]
    relays = [z_relays(i, f, n) for i, (f, n, _) in enumerate(z_parts)]
    x_relays = [x_relay(i) for i in range(6)]

    def own_units(work):
        work(0, 8, 35)
        work(8, 1, 87)

    def x_arrived(i):
        x_copies[i].wait_recv()
        x_relays[i].start()
        pack(*z_parts[i + 1])
        for c in z_all[i + 1]:
            c.start()

    def x_complete(i):
        x_relays[i].wait_recv()
        _, e, n, _ = x_parts[i]
        convert_own(e - e % 2 if e > 90 and n == 7 else e - n % 2, n + n % 2)

    def z_arrived(i):
        for d in range(2):
            z_all[i][d].wait_recv()
            relays[i][d].start()

    def z_complete(i):
        for d in range(2):
            relays[i][d].wait_recv()
        if i:
            convert_edges(*z_parts[i])
        else:
            own_units(convert_edges)

    own_units(pack)
    for c in z_all[0]:
        c.start()

    @pl.loop(0, EXT)
    def _(x):
        xr[x, 60:64, :] = jnp.zeros((4, 128), F32)
        xr[x, 124:128, :] = jnp.zeros((4, 128), F32)

    @pl.loop(0, 2 * UNITS)
    def _(t):
        for d in range(2):
            zrecv[d, t, 60:64, :] = jnp.zeros((4, 128), F32)
            zrecv[d, t, 124:128, :] = jnp.zeros((4, 128), F32)

    s_ref[...] = jnp.zeros(s_ref.shape, F32)
    pl.semaphore_wait(ready, 3)

    @pl.loop(1, GX)
    def _(k):
        root_copy(k).start()

    own_d2d.wait_recv()
    convert_own(HALO, BX)
    x_arrived(0)
    x_arrived(1)
    z_arrived(0)
    x_complete(0)
    x_complete(1)
    z_complete(0)
    x_arrived(2)
    x_arrived(3)
    z_arrived(1)
    z_arrived(2)
    x_complete(2)
    x_complete(3)
    z_complete(1)
    z_complete(2)
    x_arrived(4)
    x_arrived(5)
    z_arrived(3)
    z_arrived(4)
    x_complete(4)
    x_complete(5)

    @pl.loop(1, GX)
    def _(k):
        root_copy(k).wait_recv()

    roots_copy = pltpu.make_async_copy(roots, roots_s, local_sem.at[1])
    roots_copy.start()
    z_complete(3)
    z_complete(4)
    z_arrived(5)
    z_arrived(6)
    z_complete(5)
    z_complete(6)
    roots_copy.wait()

    mx = mxt[...]
    roll_lane = lax.broadcasted_iota(jnp.int32, (SX, 128), 1)
    relay_legs = {k: leg for k, leg, _ in RELAYED}

    def f_copy(i):
        k = ORDER[i]
        if k in relay_legs:
            j = [r[0] for r in RELAYED].index(k)
            return remote(fields.at[i], relay.at[j], f_send.at[i], r_recv.at[j], line(shifted(relay_legs[k])))
        return remote(fields.at[i], fields.at[GX + i], f_send.at[i], f_recv.at[i], line(shifted(k)))

    def forward(j):
        k, _, leg = RELAYED[j]
        i = ORDER.index(k)
        return remote(relay.at[j], fields.at[GX + i], r_send.at[j], f_recv.at[i], line(shifted(leg)))

    def arrival(i):
        return remote(fields.at[i], fields.at[GX + i], f_send.at[i], f_recv.at[i], line(shifted(1)))

    def choose(i, values):
        total = jnp.int32(0)
        for c, v in enumerate(values):
            total = jnp.where(i == c, v, total)
        return total

    def field(i):
        k = choose(i, ORDER)
        back = ((4 - k // 4) % 4) * 4 + (4 - k % 4) % 4
        rx, ry, rz = jnp.int32(0), jnp.int32(0), jnp.int32(0)
        for s in range(SLOTS):
            fx = roots_s[back, 0, s]
            mine_too = (fx + HALO) % NX // BX == me
            rx = jnp.where(mine_too, fx, rx)
            ry = jnp.where(mine_too, roots_s[back, 1, s], ry)
            rz = jnp.where(mine_too, roots_s[back, 2, s], rz)
        sx = jnp.minimum((rx + HALO - me * BX + NX) % NX, BX - 1)
        sy = ry
        sz = (rz - plane * BZ + NZ) % 256
        my_t = jnp.concatenate([ytab[pl.ds(NY - sy, 64), :], ytab[pl.ds(NY + BY - sy, 64), :]], axis=0)
        my_hi, my_lo = split(my_t.T[0:G, :])
        my_ref[0:G, 0:128] = my_hi
        my_ref[0:G, 128:256] = my_hi
        my_ref[G : 2 * G, 0:128] = my_lo
        my_ref[G : 2 * G, 128:256] = my_lo
        z_hi, z_lo = split(ztab[pl.ds(256 - sz, 256), :])
        w_ref[:, 0:128] = z_hi
        w_ref[:, 128:256] = z_lo

        both = my_ref[...]
        for g in range(BOX // GROUP):
            for j in range(GROUP):
                t = dot(both, e_ref[sx + GROUP * g + j])
                hi, lo = split(t[:G] + t[G:])
                rows = pl.ds((GROUP * g + j) * G, G)
                t1h[rows, :] = hi
                t1l[rows, :] = lo
            rows = pl.ds(GROUP * g * G, GROUP * G)
            q = dot(t1h[rows, :], w_ref[...])
            t = q[:, :128] + q[:, 128:] + dot(t1l[rows, :], w_ref[:, 0:128])
            for j in range(GROUP):
                s_ref[pl.ds(GROUP * g + j, G, stride=SX), :] = t[G * j : G * j + G]

        for g in range(6):
            tiles = [jnp.zeros((SX, 128), F32) for _ in range(3)]
            for b in range(8):
                off = 48 * b % 128
                at = 48 * b // 128
                v = s_ref[pl.ds((8 * g + b) * SX, SX), :]
                if off:
                    v = pltpu.roll(v, off, 1)
                if off + 48 > 128:
                    tiles[at] = tiles[at] + jnp.where(roll_lane >= off, v, 0.0)
                    tiles[at + 1] = tiles[at + 1] + jnp.where(roll_lane < off, v, 0.0)
                else:
                    tiles[at] = tiles[at] + v
            r = jnp.concatenate([jnp.concatenate(tiles, axis=1), jnp.zeros((8, 384), F32)], axis=0)
            hi, lo = split(r)
            o = dot(mx, jnp.concatenate([hi, lo], axis=0))
            o = o[:G] + o[G:]
            for t in range(3):
                fields[i, pl.ds(3 * g + t, G, stride=18), :] = o[:, 128 * t : 128 * t + 128]

    @pl.loop(0, GX)
    def _(i):
        field(i)
        for c in range(GX - 1):

            @pl.when(i == c)
            def _():
                f_copy(c).start()
                for j, at in enumerate(FORWARD):
                    if at == c:
                        f_copy(ORDER.index(RELAYED[j][0])).wait_recv()
                        forward(j).start()

    for i in range(GX - 1):
        arrival(i).wait_recv()

    for s in range(SLOTS):
        anchor = (roots_s[0, 0, s] + HALO) % NX // BX
        k = ((my_y - anchor // 4 + 4) % 4) * 4 + (my_x - anchor % 4 + 4) % 4
        at = choose(k, [GX + ORDER.index(c) if c else ORDER.index(0) for c in range(GX)])
        out[pl.ds(s, FLAT, stride=4), :] = fields[at]

    for i in range(GX - 1):
        f_copy(i).wait_send()
    for j in range(len(RELAYED)):
        forward(j).wait_send()

    @pl.loop(1, GX)
    def _(k):
        root_copy(k).wait_send()

    own_d2d.wait_send()
    for i in range(6):
        x_copies[i].wait_send()
        x_relays[i].wait_send()
    for i in range(7):
        for d in range(2):
            z_all[i][d].wait_send()
            relays[i][d].wait_send()


def body(potential, frag_root):
    ytab, ztab, mx = tables()
    mx = jnp.asarray(mx)
    mx_hi, mx_lo = split(mx)
    zero = jnp.zeros((G, 8), BF16)
    mxt = jnp.concatenate(
        [jnp.concatenate([m, zero, m, zero], axis=1) for m in (mx_hi, mx_lo)], axis=0
    )
    vmem = pl.BlockSpec(memory_space=pltpu.VMEM)
    dma = pltpu.SemaphoreType.DMA
    out = pl.pallas_call(
        kernel,
        out_shape=jax.ShapeDtypeStruct((FLAT * SLOTS, 128), F32),
        in_specs=[pl.BlockSpec(memory_space=pl.ANY), vmem, vmem, vmem, vmem],
        out_specs=vmem,
        scratch_shapes=[
            pltpu.VMEM((GX, 3, SLOTS), jnp.int32),
            pltpu.SMEM((GX, 3, SLOTS), jnp.int32),
            pltpu.VMEM((EXT, YL, 128), F32),
            pltpu.VMEM((2, 2 * UNITS, 64, 128), F32),
            pltpu.VMEM((2, 2 * UNITS, YL, 128), F32),
            pltpu.VMEM((EXT, 2 * YL, 256), BF16),
            pltpu.VMEM((256, 256), BF16),
            pltpu.VMEM((2 * G, 2 * YL), BF16),
            pltpu.VMEM((BOX * G, 256), BF16),
            pltpu.VMEM((BOX * G, 256), BF16),
            pltpu.VMEM((G * SX, 128), F32),
            pltpu.VMEM((2 * GX, FLAT, 128), F32),
            pltpu.VMEM((len(RELAYED), FLAT, 128), F32),
            pltpu.SemaphoreType.REGULAR, dma((GX,)), dma((GX,)), dma((2,)), dma((2,)),
            dma((6,)), dma((6,)), dma((6,)), dma((6,)),
            dma((7, 2)), dma((7, 2)), dma((7, 2)), dma((7, 2)),
            dma((GX,)), dma((GX,)), dma((4,)), dma((4,)),
        ],
        compiler_params=pltpu.CompilerParams(
            collective_id=0, has_side_effects=True, vmem_limit_bytes=66 * 1000 * 1000
        ),
    )(potential, frag_root, jnp.asarray(ytab), jnp.asarray(ztab), mxt)
    return out.reshape(FLAT, SLOTS, 128).transpose(1, 0, 2).reshape(SLOTS, FLAT * 128)


def solution(mesh):
    return jax.shard_map(
        body,
        mesh=mesh,
        in_specs=(P("gx", "gy", "gz"), P(None, ("gx", "gy", "gz"))),
        out_specs=P(("gx", "gy", "gz"), None),
        check_vma=False,
    )
```

```python
import functools

import jax
import jax.numpy as jnp
import numpy as np
from jax import lax
from jax.experimental import pallas as pl
from jax.experimental.pallas import tpu as pltpu
from jax.sharding import PartitionSpec as P

MESH = pl.DeviceIdType.MESH
G = 48
BOX = 68
HALO = 34
BX = 60
BY = 60
BZ = 128
NX = 960
NY = 120
NZ = 512
GX = 16
SLOTS = 4
EXT = 128
YL = 128
FLAT = 864
SX = 72
ORDER = (10, 6, 14, 9, 11, 5, 15, 7, 13, 2, 8, 1, 3, 4, 12, 0)
RELAYED = ((6, 5, 1), (14, 15, 3), (9, 5, 4), (11, 15, 12))
FORWARD = (7, 8, 9, 10)
GROUP = 17
UNITS = 19
OFFSETS = (0, 34, 68, 102, 8, 42, 76)
F32 = jnp.float32
BF16 = jnp.bfloat16


def interp_matrix():
    a = np.arange(G)[:, None]
    x = np.arange(BOX)[None, :]
    total = np.ones((G, BOX))
    for k in range(1, G // 2):
        total = total + 2.0 * np.cos(2.0 * np.pi * k * (a / G - x / BOX))
    return (total / BOX).astype(np.float32)


def tables():
    m = interp_matrix()
    ytab = np.zeros((248, 128), np.float32)
    for j in range(248):
        if j % NY < BOX:
            ytab[j, :G] = m[:, j % NY]
    ztab = np.zeros((512, 128), np.float32)
    for j in range(512):
        if j % 256 < BOX:
            ztab[j, :G] = m[:, j % 256]
    mx = np.zeros((G, SX), np.float32)
    mx[:, :BOX] = m
    return ytab, ztab, mx


def split(v):
    hi = v.astype(BF16)
    return hi, (v - hi.astype(F32)).astype(BF16)


def dot(a, b):
    return jnp.dot(a, b, preferred_element_type=F32)


def kernel(
    pot, root, ytab, ztab, mxt, out,
    roots, roots_s, xr, zsend, zrecv, e_ref, w_ref, my_ref, t1h, t1l, s_ref, fields, relay,
    ready, root_send, root_recv, local_sem, own_sem, x_send, x_recv, xd_send, xd_recv,
    z_send, z_recv, zd_send, zd_recv, f_send, f_recv, r_send, r_recv,
):
    me = lax.axis_index("gx")
    core = lax.axis_index("gy")
    plane = lax.axis_index("gz")
    my_y, my_x = me // 4, me % 4

    def line(g):
        return {"gx": g, "gy": core, "gz": plane}

    def shifted(k):
        return ((my_y + k // 4) % 4) * 4 + (my_x + k % 4) % 4

    nxt, prv = (me + 1) % GX, (me + GX - 1) % GX
    partner = {"gx": me, "gy": 1 - core, "gz": plane}
    z_up = {"gx": me, "gy": core, "gz": (plane + 1) % 4}
    z_down = {"gx": me, "gy": core, "gz": (plane + 3) % 4}

    barrier = pltpu.get_barrier_semaphore()
    first = [partner, z_up, z_down, line(nxt), line(prv)] + [line(shifted(k)) for k in (1, 2, 3, 4, 8, 12)]
    for d in first:
        pl.semaphore_signal(barrier, inc=1, device_id=d, device_id_type=MESH)
    mine = pl.ds(pl.multiple_of(core * 64, 64), BY)

    local = pltpu.make_async_copy(pot, xr.at[pl.ds(HALO, BX), mine], local_sem.at[0])
    local.start()
    lane = lax.broadcasted_iota(jnp.int32, (32, 128), 1)

    def pack(first, count, slab):
        @pl.loop(0, count)
        def _(u):
            for part in range(2):
                here = pl.ds(pl.multiple_of(core * 64 + 32 * part, 32), 32)
                tiles = [[jnp.zeros((32, 128), F32) for _ in range(2)] for _ in range(2)]
                for j, off in enumerate(OFFSETS):
                    v = xr[slab + 7 * u + j, here, :]
                    for d, at in enumerate((off - 94, off)):
                        w = pltpu.roll(v, at % 128, 1) if at % 128 else v
                        if j == 3:
                            tiles[d][0] = jnp.where(lane >= off, w, tiles[d][0])
                            tiles[d][1] = jnp.where(lane < off + 34 - 128, w, tiles[d][1])
                        else:
                            inside = (lane >= off) & (lane < off + 34)
                            tiles[d][j // 4] = jnp.where(inside, w, tiles[d][j // 4])
                for d in range(2):
                    for t in range(2):
                        zsend[d, 2 * (first + u) + t, 32 * part : 32 * part + 32] = tiles[d][t]

    def own_units(work):
        work(0, 8, 35)
        work(8, 1, 87)

    local.wait()
    own_units(pack)
    pl.semaphore_wait(barrier, len(first))
    for k in (4, 8, 12):
        pl.semaphore_signal(ready, inc=1, device_id=line(shifted(k)), device_id_type=MESH)

    def remote(src, dst, ssem, rsem, to):
        return pltpu.make_async_remote_copy(
            src_ref=src, dst_ref=dst, send_sem=ssem, recv_sem=rsem, device_id=to, device_id_type=MESH
        )

    x_parts = (
        (26, 0, 14, nxt), (0, 94, 13, prv), (40, 14, 14, nxt), (13, 107, 14, prv), (54, 28, 6, nxt), (27, 121, 7, prv)
    )
    x_copies = [
        remote(pot.at[pl.ds(s, n)], xr.at[pl.ds(e, n), mine], x_send.at[i], x_recv.at[i], line(to))
        for i, (s, e, n, to) in enumerate(x_parts)
    ]
    def root_copy(k):
        return remote(root, roots.at[k], root_send.at[k], root_recv.at[k], line(shifted(k)))

    for c in x_copies:
        c.start()
    own_d2d = remote(pot, xr.at[pl.ds(HALO, BX), mine], own_sem.at[0], own_sem.at[1], partner)
    own_d2d.start()
    roots[0] = root[...]

    def z_copies(i, first, count):
        rows = pl.ds(2 * first, 2 * count)
        return [
            remote(zsend.at[d, rows, 0:BY], zrecv.at[d, rows, mine], z_send.at[i, d], z_recv.at[i, d], to)
            for d, to in enumerate((z_up, z_down))
        ]

    def z_relays(i, first, count):
        rows = pl.ds(2 * first, 2 * count)
        return [
            remote(zrecv.at[d, rows, mine], zrecv.at[d, rows, mine], zd_send.at[i, d], zd_recv.at[i, d], partner)
            for d in range(2)
        ]

    def x_relay(i):
        _, e, n, _ = x_parts[i]
        return remote(xr.at[pl.ds(e, n), mine], xr.at[pl.ds(e, n), mine], xd_send.at[i], xd_recv.at[i], partner)

    def convert_own(slab, count):
        @pl.loop(0, count // 2)
        def _(p):
            for j in range(2):
                x = slab + 2 * p + j
                h, l = split(xr[x])
                e_ref[x, 0:128, 0:128] = h
                e_ref[x, 128:256, 0:128] = l

    def convert_edges(first, count, slab):
        @pl.loop(0, count)
        def _(u):
            for part in range(4):
                here = pl.ds(32 * part, 32)
                below = [zrecv[0, 2 * (first + u) + t, here, :] for t in range(2)]
                above = [zrecv[1, 2 * (first + u) + t, here, :] for t in range(2)]
                for j, off in enumerate(OFFSETS):
                    x = slab + 7 * u + j
                    both = []
                    for tiles, at in ((above, -off), (below, 94 - off)):
                        v = jnp.where(lane >= off, tiles[0], tiles[1]) if j == 3 else tiles[j // 4]
                        both.append(pltpu.roll(v, at % 128, 1) if at % 128 else v)
                    h, l = split(jnp.where(lane < 34, both[0], jnp.where(lane >= 94, both[1], 0.0)))
                    e_ref[x, 32 * part : 32 * part + 32, 128:256] = h
                    e_ref[x, 128 + 32 * part : 160 + 32 * part, 128:256] = l

    z_parts = ((0, 9, 35), (9, 2, 0), (11, 2, 93), (13, 2, 14), (15, 2, 107), (17, 1, 28), (18, 1, 121))
    z_all = [z_copies(i, f, n) for i, (f, n, _) in enumerate(z_parts)]
    relays = [z_relays(i, f, n) for i, (f, n, _) in enumerate(z_parts)]
    x_relays = [x_relay(i) for i in range(6)]

    def x_arrived(i):
        x_copies[i].wait_recv()
        x_relays[i].start()
        pack(*z_parts[i + 1])
        for c in z_all[i + 1]:
            c.start()

    def x_complete(i):
        x_relays[i].wait_recv()
        _, e, n, _ = x_parts[i]
        convert_own(e - e % 2 if e > 90 and n == 7 else e - n % 2, n + n % 2)

    def z_arrived(i):
        for d in range(2):
            z_all[i][d].wait_recv()
            relays[i][d].start()

    def z_complete(i):
        for d in range(2):
            relays[i][d].wait_recv()
        if i:
            convert_edges(*z_parts[i])
        else:
            own_units(convert_edges)

    for c in z_all[0]:
        c.start()

    @pl.loop(0, EXT)
    def _(x):
        xr[x, 60:64, :] = jnp.zeros((4, 128), F32)
        xr[x, 124:128, :] = jnp.zeros((4, 128), F32)

    @pl.loop(0, 2 * UNITS)
    def _(t):
        for d in range(2):
            zrecv[d, t, 60:64, :] = jnp.zeros((4, 128), F32)
            zrecv[d, t, 124:128, :] = jnp.zeros((4, 128), F32)

    s_ref[...] = jnp.zeros(s_ref.shape, F32)
    pl.semaphore_wait(ready, 3)

    @pl.loop(1, GX)
    def _(k):
        root_copy(k).start()

    own_d2d.wait_recv()
    convert_own(HALO, BX)
    x_arrived(0)
    x_arrived(1)
    z_arrived(0)
    x_complete(0)
    x_complete(1)
    z_complete(0)
    x_arrived(2)
    x_arrived(3)
    z_arrived(1)
    z_arrived(2)
    x_complete(2)
    x_complete(3)
    z_complete(1)
    z_complete(2)
    x_arrived(4)
    x_arrived(5)
    z_arrived(3)
    z_arrived(4)
    x_complete(4)
    x_complete(5)

    @pl.loop(1, GX)
    def _(k):
        root_copy(k).wait_recv()

    roots_copy = pltpu.make_async_copy(roots, roots_s, local_sem.at[1])
    roots_copy.start()
    z_complete(3)
    z_complete(4)
    z_arrived(5)
    z_arrived(6)
    z_complete(5)
    z_complete(6)
    roots_copy.wait()

    mx = mxt[...]
    roll_lane = lax.broadcasted_iota(jnp.int32, (SX, 128), 1)
    relay_legs = {k: leg for k, leg, _ in RELAYED}

    def f_copy(i):
        k = ORDER[i]
        if k in relay_legs:
            j = [r[0] for r in RELAYED].index(k)
            return remote(fields.at[i], relay.at[j], f_send.at[i], r_recv.at[j], line(shifted(relay_legs[k])))
        return remote(fields.at[i], fields.at[GX + i], f_send.at[i], f_recv.at[i], line(shifted(k)))

    def forward(j):
        k, _, leg = RELAYED[j]
        i = ORDER.index(k)
        return remote(relay.at[j], fields.at[GX + i], r_send.at[j], f_recv.at[i], line(shifted(leg)))

    def arrival(i):
        return remote(fields.at[i], fields.at[GX + i], f_send.at[i], f_recv.at[i], line(shifted(1)))

    def choose(i, values):
        total = jnp.int32(0)
        for c, v in enumerate(values):
            total = jnp.where(i == c, v, total)
        return total

    def field(i):
        k = choose(i, ORDER)
        back = ((4 - k // 4) % 4) * 4 + (4 - k % 4) % 4
        rx, ry, rz = jnp.int32(0), jnp.int32(0), jnp.int32(0)
        for s in range(SLOTS):
            fx = roots_s[back, 0, s]
            mine_too = (fx + HALO) % NX // BX == me
            rx = jnp.where(mine_too, fx, rx)
            ry = jnp.where(mine_too, roots_s[back, 1, s], ry)
            rz = jnp.where(mine_too, roots_s[back, 2, s], rz)
        sx = jnp.minimum((rx + HALO - me * BX + NX) % NX, BX - 1)
        sy = ry
        sz = (rz - plane * BZ + NZ) % 256
        my_t = jnp.concatenate([ytab[pl.ds(NY - sy, 64), :], ytab[pl.ds(NY + BY - sy, 64), :]], axis=0)
        my_hi, my_lo = split(my_t.T[0:G, :])
        my_ref[0:G, 0:128] = my_hi
        my_ref[0:G, 128:256] = my_hi
        my_ref[G : 2 * G, 0:128] = my_lo
        my_ref[G : 2 * G, 128:256] = my_lo
        z_hi, z_lo = split(ztab[pl.ds(256 - sz, 256), :])
        w_ref[:, 0:128] = z_hi
        w_ref[:, 128:256] = z_lo

        both = my_ref[...]
        for g in range(BOX // GROUP):
            for j in range(GROUP):
                t = dot(both, e_ref[sx + GROUP * g + j])
                hi, lo = split(t[:G] + t[G:])
                rows = pl.ds((GROUP * g + j) * G, G)
                t1h[rows, :] = hi
                t1l[rows, :] = lo
            rows = pl.ds(GROUP * g * G, GROUP * G)
            q = dot(t1h[rows, :], w_ref[...])
            t = q[:, :128] + q[:, 128:] + dot(t1l[rows, :], w_ref[:, 0:128])
            for j in range(GROUP):
                s_ref[pl.ds(GROUP * g + j, G, stride=SX), :] = t[G * j : G * j + G]

        for g in range(6):
            tiles = [jnp.zeros((SX, 128), F32) for _ in range(3)]
            for b in range(8):
                off = 48 * b % 128
                at = 48 * b // 128
                v = s_ref[pl.ds((8 * g + b) * SX, SX), :]
                if off:
                    v = pltpu.roll(v, off, 1)
                if off + 48 > 128:
                    tiles[at] = tiles[at] + jnp.where(roll_lane >= off, v, 0.0)
                    tiles[at + 1] = tiles[at + 1] + jnp.where(roll_lane < off, v, 0.0)
                else:
                    tiles[at] = tiles[at] + v
            r = jnp.concatenate([jnp.concatenate(tiles, axis=1), jnp.zeros((8, 384), F32)], axis=0)
            hi, lo = split(r)
            o = dot(mx, jnp.concatenate([hi, lo], axis=0))
            o = o[:G] + o[G:]
            for t in range(3):
                fields[i, pl.ds(3 * g + t, G, stride=18), :] = o[:, 128 * t : 128 * t + 128]

    @pl.loop(0, GX)
    def _(i):
        field(i)
        for c in range(GX - 1):

            @pl.when(i == c)
            def _():
                f_copy(c).start()
                for j, at in enumerate(FORWARD):
                    if at == c:
                        f_copy(ORDER.index(RELAYED[j][0])).wait_recv()
                        forward(j).start()

    for i in range(GX - 1):
        arrival(i).wait_recv()

    for s in range(SLOTS):
        anchor = (roots_s[0, 0, s] + HALO) % NX // BX
        k = ((my_y - anchor // 4 + 4) % 4) * 4 + (my_x - anchor % 4 + 4) % 4
        at = choose(k, [GX + ORDER.index(c) if c else ORDER.index(0) for c in range(GX)])
        out[pl.ds(s, FLAT, stride=4), :] = fields[at]

    for i in range(GX - 1):
        f_copy(i).wait_send()
    for j in range(len(RELAYED)):
        forward(j).wait_send()

    @pl.loop(1, GX)
    def _(k):
        root_copy(k).wait_send()

    own_d2d.wait_send()
    for i in range(6):
        x_copies[i].wait_send()
        x_relays[i].wait_send()
    for i in range(7):
        for d in range(2):
            z_all[i][d].wait_send()
            relays[i][d].wait_send()


def body(potential, frag_root):
    ytab, ztab, mx = tables()
    mx = jnp.asarray(mx)
    mx_hi, mx_lo = split(mx)
    zero = jnp.zeros((G, 8), BF16)
    mxt = jnp.concatenate(
        [jnp.concatenate([m, zero, m, zero], axis=1) for m in (mx_hi, mx_lo)], axis=0
    )
    vmem = pl.BlockSpec(memory_space=pltpu.VMEM)
    dma = pltpu.SemaphoreType.DMA
    out = pl.pallas_call(
        kernel,
        out_shape=jax.ShapeDtypeStruct((FLAT * SLOTS, 128), F32),
        in_specs=[pl.BlockSpec(memory_space=pl.ANY), vmem, vmem, vmem, vmem],
        out_specs=vmem,
        scratch_shapes=[
            pltpu.VMEM((GX, 3, SLOTS), jnp.int32),
            pltpu.SMEM((GX, 3, SLOTS), jnp.int32),
            pltpu.VMEM((EXT, YL, 128), F32),
            pltpu.VMEM((2, 2 * UNITS, 64, 128), F32),
            pltpu.VMEM((2, 2 * UNITS, YL, 128), F32),
            pltpu.VMEM((EXT, 2 * YL, 256), BF16),
            pltpu.VMEM((256, 256), BF16),
            pltpu.VMEM((2 * G, 2 * YL), BF16),
            pltpu.VMEM((BOX * G, 256), BF16),
            pltpu.VMEM((BOX * G, 256), BF16),
            pltpu.VMEM((G * SX, 128), F32),
            pltpu.VMEM((2 * GX, FLAT, 128), F32),
            pltpu.VMEM((len(RELAYED), FLAT, 128), F32),
            pltpu.SemaphoreType.REGULAR, dma((GX,)), dma((GX,)), dma((2,)), dma((2,)),
            dma((6,)), dma((6,)), dma((6,)), dma((6,)),
            dma((7, 2)), dma((7, 2)), dma((7, 2)), dma((7, 2)),
            dma((GX,)), dma((GX,)), dma((4,)), dma((4,)),
        ],
        compiler_params=pltpu.CompilerParams(
            collective_id=0, has_side_effects=True, vmem_limit_bytes=66 * 1000 * 1000
        ),
    )(potential, frag_root, jnp.asarray(ytab), jnp.asarray(ztab), mxt)
    return out.reshape(FLAT, SLOTS, 128).transpose(1, 0, 2).reshape(SLOTS, FLAT * 128)


def solution(mesh):
    return jax.shard_map(
        body,
        mesh=mesh,
        in_specs=(P("gx", "gy", "gz"), P(None, ("gx", "gy", "gz"))),
        out_specs=P(("gx", "gy", "gz"), None),
        check_vma=False,
    )
```

```python
import functools

import jax
import jax.numpy as jnp
import numpy as np
from jax import lax
from jax.experimental import pallas as pl
from jax.experimental.pallas import tpu as pltpu
from jax.sharding import PartitionSpec as P

MESH = pl.DeviceIdType.MESH
G = 48
BOX = 68
HALO = 34
BX = 60
BY = 60
BZ = 128
NX = 960
NY = 120
NZ = 512
GX = 16
SLOTS = 4
EXT = 128
YL = 128
FLAT = 864
PLANE = 18
SENT = FLAT - PLANE
SX = 72
ORDER = (10, 6, 14, 9, 11, 5, 15, 7, 13, 2, 8, 1, 3, 4, 12, 0)
RELAYED = ((6, 5, 1), (14, 15, 3), (9, 5, 4), (11, 15, 12))
FORWARD = (7, 8, 9, 10)
GROUP = 17
UNITS = 19
OFFSETS = (0, 34, 68, 102, 8, 42, 76)
F32 = jnp.float32
BF16 = jnp.bfloat16


def interp_matrix():
    a = np.arange(G)[:, None]
    x = np.arange(BOX)[None, :]
    total = np.ones((G, BOX))
    for k in range(1, G // 2):
        total = total + 2.0 * np.cos(2.0 * np.pi * k * (a / G - x / BOX))
    return (total / BOX).astype(np.float32)


def tables():
    m = interp_matrix()
    ytab = np.zeros((248, 128), np.float32)
    for j in range(248):
        if j % NY < BOX:
            ytab[j, :G] = m[:, j % NY]
    ztab = np.zeros((512, 128), np.float32)
    for j in range(512):
        if j % 256 < BOX:
            ztab[j, :G] = m[:, j % 256]
    mx = np.zeros((G, SX), np.float32)
    mx[:, :BOX] = m
    return ytab, ztab, mx


def split(v):
    hi = v.astype(BF16)
    return hi, (v - hi.astype(F32)).astype(BF16)


def dot(a, b):
    return jnp.dot(a, b, preferred_element_type=F32)


def kernel(
    pot, root, ytab_in, ztab_in, mxt_in, out,
    ytab, ztab, mxt, stage, roots, roots_s, xr, zsend, zrecv, e_ref, w_ref, my_ref, t1h, t1l, s_ref, fields, relay,
    table_sem, out_sem, ready, root_send, root_recv, local_sem, own_sem, x_send, x_recv, xd_send, xd_recv,
    z_send, z_recv, zd_send, zd_recv, f_send, f_recv, r_send, r_recv,
):
    tables_in = [
        pltpu.make_async_copy(a, b, table_sem.at[i])
        for i, (a, b) in enumerate(((ytab_in, ytab), (ztab_in, ztab), (mxt_in, mxt), (root, roots.at[0])))
    ]
    me = lax.axis_index("gx")
    core = lax.axis_index("gy")
    plane = lax.axis_index("gz")
    my_y, my_x = me // 4, me % 4

    def line(g):
        return {"gx": g, "gy": core, "gz": plane}

    def shifted(k):
        return ((my_y + k // 4) % 4) * 4 + (my_x + k % 4) % 4

    nxt, prv = (me + 1) % GX, (me + GX - 1) % GX
    partner = {"gx": me, "gy": 1 - core, "gz": plane}
    z_up = {"gx": me, "gy": core, "gz": (plane + 1) % 4}
    z_down = {"gx": me, "gy": core, "gz": (plane + 3) % 4}

    barrier = pltpu.get_barrier_semaphore()
    first = [partner, z_up, z_down, line(nxt), line(prv)] + [line(shifted(k)) for k in (1, 2, 3, 4, 8, 12)]
    for d in first:
        pl.semaphore_signal(barrier, inc=1, device_id=d, device_id_type=MESH)
    mine = pl.ds(pl.multiple_of(core * 64, 64), BY)

    local = pltpu.make_async_copy(pot, xr.at[pl.ds(HALO, BX), mine], local_sem.at[0])
    local.start()
    lane = lax.broadcasted_iota(jnp.int32, (32, 128), 1)

    def pack(first, count, slab):
        @pl.loop(0, count)
        def _(u):
            for part in range(2):
                here = pl.ds(pl.multiple_of(core * 64 + 32 * part, 32), 32)
                tiles = [[jnp.zeros((32, 128), F32) for _ in range(2)] for _ in range(2)]
                for j, off in enumerate(OFFSETS):
                    v = xr[slab + 7 * u + j, here, :]
                    for d, at in enumerate((off - 94, off)):
                        w = pltpu.roll(v, at % 128, 1) if at % 128 else v
                        if j == 3:
                            tiles[d][0] = jnp.where(lane >= off, w, tiles[d][0])
                            tiles[d][1] = jnp.where(lane < off + 34 - 128, w, tiles[d][1])
                        else:
                            inside = (lane >= off) & (lane < off + 34)
                            tiles[d][j // 4] = jnp.where(inside, w, tiles[d][j // 4])
                for d in range(2):
                    for t in range(2):
                        zsend[d, 2 * (first + u) + t, 32 * part : 32 * part + 32] = tiles[d][t]

    def own_units(work):
        work(0, 8, 35)
        work(8, 1, 87)

    for c in tables_in:
        c.start()
    local.wait()
    own_units(pack)
    pl.semaphore_wait(barrier, len(first))
    for k in (4, 8, 12):
        pl.semaphore_signal(ready, inc=1, device_id=line(shifted(k)), device_id_type=MESH)

    def remote(src, dst, ssem, rsem, to):
        return pltpu.make_async_remote_copy(
            src_ref=src, dst_ref=dst, send_sem=ssem, recv_sem=rsem, device_id=to, device_id_type=MESH
        )

    x_parts = (
        (26, 0, 14, nxt), (0, 94, 13, prv), (40, 14, 14, nxt), (13, 107, 14, prv), (54, 28, 6, nxt), (27, 121, 7, prv)
    )
    x_copies = [
        remote(pot.at[pl.ds(s, n)], xr.at[pl.ds(e, n), mine], x_send.at[i], x_recv.at[i], line(to))
        for i, (s, e, n, to) in enumerate(x_parts)
    ]
    def root_copy(k):
        return remote(root, roots.at[k], root_send.at[k], root_recv.at[k], line(shifted(k)))

    for c in x_copies:
        c.start()
    own_d2d = remote(pot, xr.at[pl.ds(HALO, BX), mine], own_sem.at[0], own_sem.at[1], partner)
    own_d2d.start()

    def z_copies(i, first, count):
        rows = pl.ds(2 * first, 2 * count)
        return [
            remote(zsend.at[d, rows, 0:BY], zrecv.at[d, rows, mine], z_send.at[i, d], z_recv.at[i, d], to)
            for d, to in enumerate((z_up, z_down))
        ]

    def z_relays(i, first, count):
        rows = pl.ds(2 * first, 2 * count)
        return [
            remote(zrecv.at[d, rows, mine], zrecv.at[d, rows, mine], zd_send.at[i, d], zd_recv.at[i, d], partner)
            for d in range(2)
        ]

    def x_relay(i):
        _, e, n, _ = x_parts[i]
        return remote(xr.at[pl.ds(e, n), mine], xr.at[pl.ds(e, n), mine], xd_send.at[i], xd_recv.at[i], partner)

    def convert_own(slab, count):
        @pl.loop(0, count // 2)
        def _(p):
            for j in range(2):
                x = slab + 2 * p + j
                h, l = split(xr[x])
                e_ref[x, 0:128, 0:128] = h
                e_ref[x, 128:256, 0:128] = l

    def convert_edges(first, count, slab):
        @pl.loop(0, count)
        def _(u):
            for part in range(4):
                here = pl.ds(32 * part, 32)
                below = [zrecv[0, 2 * (first + u) + t, here, :] for t in range(2)]
                above = [zrecv[1, 2 * (first + u) + t, here, :] for t in range(2)]
                for j, off in enumerate(OFFSETS):
                    x = slab + 7 * u + j
                    both = []
                    for tiles, at in ((above, -off), (below, 94 - off)):
                        v = jnp.where(lane >= off, tiles[0], tiles[1]) if j == 3 else tiles[j // 4]
                        both.append(pltpu.roll(v, at % 128, 1) if at % 128 else v)
                    h, l = split(jnp.where(lane < 34, both[0], jnp.where(lane >= 94, both[1], 0.0)))
                    e_ref[x, 32 * part : 32 * part + 32, 128:256] = h
                    e_ref[x, 128 + 32 * part : 160 + 32 * part, 128:256] = l

    z_parts = ((0, 9, 35), (9, 2, 0), (11, 2, 93), (13, 2, 14), (15, 2, 107), (17, 1, 28), (18, 1, 121))
    z_all = [z_copies(i, f, n) for i, (f, n, _) in enumerate(z_parts)]
    relays = [z_relays(i, f, n) for i, (f, n, _) in enumerate(z_parts)]
    x_relays = [x_relay(i) for i in range(6)]

    def x_arrived(i):
        x_copies[i].wait_recv()
        x_relays[i].start()
        pack(*z_parts[i + 1])
        for c in z_all[i + 1]:
            c.start()

    def x_complete(i):
        x_relays[i].wait_recv()
        _, e, n, _ = x_parts[i]
        convert_own(e - e % 2 if e > 90 and n == 7 else e - n % 2, n + n % 2)

    def z_arrived(i):
        for d in range(2):
            z_all[i][d].wait_recv()
            relays[i][d].start()

    def z_complete(i):
        for d in range(2):
            relays[i][d].wait_recv()
        if i:
            convert_edges(*z_parts[i])
        else:
            own_units(convert_edges)

    for c in z_all[0]:
        c.start()

    @pl.loop(0, EXT)
    def _(x):
        xr[x, 60:64, :] = jnp.zeros((4, 128), F32)
        xr[x, 124:128, :] = jnp.zeros((4, 128), F32)

    @pl.loop(0, 2 * UNITS)
    def _(t):
        for d in range(2):
            zrecv[d, t, 60:64, :] = jnp.zeros((4, 128), F32)
            zrecv[d, t, 124:128, :] = jnp.zeros((4, 128), F32)

    s_ref[...] = jnp.zeros(s_ref.shape, F32)
    pl.semaphore_wait(ready, 3)

    @pl.loop(1, GX)
    def _(k):
        root_copy(k).start()

    own_d2d.wait_recv()
    convert_own(HALO, BX)
    x_arrived(0)
    x_arrived(1)
    z_arrived(0)
    x_complete(0)
    x_complete(1)
    z_complete(0)
    x_arrived(2)
    x_arrived(3)
    z_arrived(1)
    z_arrived(2)
    x_complete(2)
    x_complete(3)
    z_complete(1)
    z_complete(2)
    x_arrived(4)
    x_arrived(5)
    z_arrived(3)
    z_arrived(4)
    x_complete(4)
    x_complete(5)

    @pl.loop(1, GX)
    def _(k):
        root_copy(k).wait_recv()

    for c in tables_in:
        c.wait()
    roots_copy = pltpu.make_async_copy(roots, roots_s, local_sem.at[1])
    roots_copy.start()
    z_complete(3)
    z_complete(4)
    z_arrived(5)
    z_arrived(6)
    z_complete(5)
    z_complete(6)
    roots_copy.wait()

    mx = mxt[...]
    roll_lane = lax.broadcasted_iota(jnp.int32, (SX, 128), 1)
    sent = pl.ds(0, SENT)
    relay_legs = {k: leg for k, leg, _ in RELAYED}

    def f_copy(i):
        k = ORDER[i]
        if k in relay_legs:
            j = [r[0] for r in RELAYED].index(k)
            return remote(fields.at[i, sent], relay.at[j], f_send.at[i], r_recv.at[j], line(shifted(relay_legs[k])))
        return remote(fields.at[i, sent], fields.at[GX + i, sent], f_send.at[i], f_recv.at[i], line(shifted(k)))

    def forward(j):
        k, _, leg = RELAYED[j]
        i = ORDER.index(k)
        return remote(relay.at[j], fields.at[GX + i, sent], r_send.at[j], f_recv.at[i], line(shifted(leg)))

    def arrival(i):
        return remote(fields.at[i, sent], fields.at[GX + i, sent], f_send.at[i], f_recv.at[i], line(shifted(1)))

    def choose(i, values):
        total = jnp.int32(0)
        for c, v in enumerate(values):
            total = jnp.where(i == c, v, total)
        return total

    def field(i):
        k = choose(i, ORDER)
        back = ((4 - k // 4) % 4) * 4 + (4 - k % 4) % 4
        rx, ry, rz = jnp.int32(0), jnp.int32(0), jnp.int32(0)
        for s in range(SLOTS):
            fx = roots_s[back, 0, s]
            mine_too = (fx + HALO) % NX // BX == me
            rx = jnp.where(mine_too, fx, rx)
            ry = jnp.where(mine_too, roots_s[back, 1, s], ry)
            rz = jnp.where(mine_too, roots_s[back, 2, s], rz)
        sx = jnp.minimum((rx + HALO - me * BX + NX) % NX, BX - 1)
        sy = ry
        sz = (rz - plane * BZ + NZ) % 256
        my_t = jnp.concatenate([ytab[pl.ds(NY - sy, 64), :], ytab[pl.ds(NY + BY - sy, 64), :]], axis=0)
        my_hi, my_lo = split(my_t.T[0:G, :])
        my_ref[0:G, 0:128] = my_hi
        my_ref[0:G, 128:256] = my_hi
        my_ref[G : 2 * G, 0:128] = my_lo
        my_ref[G : 2 * G, 128:256] = my_lo
        z_hi, z_lo = split(ztab[pl.ds(256 - sz, 256), :])
        w_ref[:, 0:128] = z_hi
        w_ref[:, 128:256] = z_lo

        both = my_ref[...]
        for g in range(BOX // GROUP):
            for j in range(GROUP):
                t = dot(both, e_ref[sx + GROUP * g + j])
                hi, lo = split(t[:G] + t[G:])
                rows = pl.ds((GROUP * g + j) * G, G)
                t1h[rows, :] = hi
                t1l[rows, :] = lo
            rows = pl.ds(GROUP * g * G, GROUP * G)
            q = dot(t1h[rows, :], w_ref[...])
            t = q[:, :128] + q[:, 128:] + dot(t1l[rows, :], w_ref[:, 0:128])
            for j in range(GROUP):
                s_ref[pl.ds(GROUP * g + j, G, stride=SX), :] = t[G * j : G * j + G]

        for g in range(6):
            tiles = [jnp.zeros((SX, 128), F32) for _ in range(3)]
            for b in range(8):
                off = 48 * b % 128
                at = 48 * b // 128
                v = s_ref[pl.ds((8 * g + b) * SX, SX), :]
                if off:
                    v = pltpu.roll(v, off, 1)
                if off + 48 > 128:
                    tiles[at] = tiles[at] + jnp.where(roll_lane >= off, v, 0.0)
                    tiles[at + 1] = tiles[at + 1] + jnp.where(roll_lane < off, v, 0.0)
                else:
                    tiles[at] = tiles[at] + v
            r = jnp.concatenate([jnp.concatenate(tiles, axis=1), jnp.zeros((8, 384), F32)], axis=0)
            hi, lo = split(r)
            o = dot(mx, jnp.concatenate([hi, lo], axis=0))
            o = o[:G] + o[G:]
            for t in range(3):
                fields[i, pl.ds(3 * g + t, G, stride=18), :] = o[:, 128 * t : 128 * t + 128]

    @pl.loop(0, GX)
    def _(i):
        field(i)
        for c in range(GX - 1):

            @pl.when(i == c)
            def _():
                f_copy(c).start()
                for j, at in enumerate(FORWARD):
                    if at == c:
                        f_copy(ORDER.index(RELAYED[j][0])).wait_recv()
                        forward(j).start()

    for i in range(GX - 1):
        arrival(i).wait_recv()

    places = []
    for s in range(SLOTS):
        anchor = (roots_s[0, 0, s] + HALO) % NX // BX
        k = ((my_y - anchor // 4 + 4) % 4) * 4 + (my_x - anchor % 4 + 4) % 4
        places.append(choose(k, [GX + ORDER.index(c) if c else ORDER.index(0) for c in range(GX)]))

    out_copies = []
    for c in range(4):
        n = 216 if c < 3 else 216 - PLANE
        for s, at in enumerate(places):
            stage[pl.ds(864 * c + s, n, stride=4), :] = fields[at, 216 * c : 216 * c + n]
            if c == 3:
                for r in range(PLANE):
                    even = fields[at, pl.ds(r, 24, stride=2 * PLANE), :]
                    odd = fields[at, pl.ds(r + PLANE, 23, stride=2 * PLANE), :]
                    last = jnp.sum(even, axis=0, keepdims=True) - jnp.sum(odd, axis=0, keepdims=True)
                    stage[pl.ds(4 * (SENT + r) + s, 1), :] = last
        rows = pl.ds(864 * c, 864)
        out_copies.append(pltpu.make_async_copy(stage.at[rows], out.at[rows], out_sem.at[c]))
        out_copies[c].start()

    for i in range(GX - 1):
        f_copy(i).wait_send()
    for j in range(len(RELAYED)):
        forward(j).wait_send()

    @pl.loop(1, GX)
    def _(k):
        root_copy(k).wait_send()

    for c in out_copies:
        c.wait()
    own_d2d.wait_send()
    for i in range(6):
        x_copies[i].wait_send()
        x_relays[i].wait_send()
    for i in range(7):
        for d in range(2):
            z_all[i][d].wait_send()
            relays[i][d].wait_send()


def body(potential, frag_root):
    ytab, ztab, mx = tables()
    mx = jnp.asarray(mx)
    mx_hi, mx_lo = split(mx)
    zero = jnp.zeros((G, 8), BF16)
    mxt = jnp.concatenate(
        [jnp.concatenate([m, zero, m, zero], axis=1) for m in (mx_hi, mx_lo)], axis=0
    )
    dma = pltpu.SemaphoreType.DMA
    out = pl.pallas_call(
        kernel,
        out_shape=jax.ShapeDtypeStruct((FLAT * SLOTS, 128), F32),
        in_specs=[pl.BlockSpec(memory_space=pl.ANY)] * 5,
        out_specs=pl.BlockSpec(memory_space=pl.ANY),
        scratch_shapes=[
            pltpu.VMEM((248, 128), F32),
            pltpu.VMEM((512, 128), F32),
            pltpu.VMEM(mxt.shape, BF16),
            pltpu.VMEM((FLAT * SLOTS, 128), F32),
            pltpu.VMEM((GX, 3, SLOTS), jnp.int32),
            pltpu.SMEM((GX, 3, SLOTS), jnp.int32),
            pltpu.VMEM((EXT, YL, 128), F32),
            pltpu.VMEM((2, 2 * UNITS, 64, 128), F32),
            pltpu.VMEM((2, 2 * UNITS, YL, 128), F32),
            pltpu.VMEM((EXT, 2 * YL, 256), BF16),
            pltpu.VMEM((256, 256), BF16),
            pltpu.VMEM((2 * G, 2 * YL), BF16),
            pltpu.VMEM((BOX * G, 256), BF16),
            pltpu.VMEM((BOX * G, 256), BF16),
            pltpu.VMEM((G * SX, 128), F32),
            pltpu.VMEM((2 * GX, FLAT, 128), F32),
            pltpu.VMEM((len(RELAYED), SENT, 128), F32),
            dma((4,)), dma((4,)),
            pltpu.SemaphoreType.REGULAR, dma((GX,)), dma((GX,)), dma((2,)), dma((2,)),
            dma((6,)), dma((6,)), dma((6,)), dma((6,)),
            dma((7, 2)), dma((7, 2)), dma((7, 2)), dma((7, 2)),
            dma((GX,)), dma((GX,)), dma((4,)), dma((4,)),
        ],
        compiler_params=pltpu.CompilerParams(
            collective_id=0, has_side_effects=True, vmem_limit_bytes=66 * 1000 * 1000
        ),
    )(potential, frag_root, jnp.asarray(ytab), jnp.asarray(ztab), mxt)
    return out.reshape(FLAT, SLOTS, 128).transpose(1, 0, 2).reshape(SLOTS, FLAT * 128)


def solution(mesh):
    return jax.shard_map(
        body,
        mesh=mesh,
        in_specs=(P("gx", "gy", "gz"), P(None, ("gx", "gy", "gz"))),
        out_specs=P(("gx", "gy", "gz"), None),
        check_vma=False,
    )
```

```python
import functools

import jax
import jax.numpy as jnp
import numpy as np
from jax import lax
from jax.experimental import pallas as pl
from jax.experimental.pallas import tpu as pltpu
from jax.sharding import PartitionSpec as P

MESH = pl.DeviceIdType.MESH
G = 48
BOX = 68
HALO = 34
BX = 60
BY = 60
BZ = 128
NX = 960
NY = 120
NZ = 512
GX = 16
SLOTS = 4
EXT = 128
YL = 128
FLAT = 864
PLANE = 18
SENT = FLAT - PLANE
SX = 72
ORDER = (10, 6, 14, 9, 11, 5, 15, 7, 13, 2, 8, 1, 3, 4, 12, 0)
RELAYED = ((6, 5, 1), (14, 15, 3), (9, 5, 4), (11, 15, 12))
FORWARD = (7, 8, 9, 10)
GROUP = 17
UNITS = 19
OFFSETS = (0, 34, 68, 102, 8, 42, 76)
F32 = jnp.float32
BF16 = jnp.bfloat16


def interp_matrix():
    a = np.arange(G)[:, None]
    x = np.arange(BOX)[None, :]
    total = np.ones((G, BOX))
    for k in range(1, G // 2):
        total = total + 2.0 * np.cos(2.0 * np.pi * k * (a / G - x / BOX))
    return (total / BOX).astype(np.float32)


def tables():
    m = interp_matrix()
    ytab = np.zeros((248, 128), np.float32)
    for j in range(248):
        if j % NY < BOX:
            ytab[j, :G] = m[:, j % NY]
    ztab = np.zeros((512, 128), np.float32)
    for j in range(512):
        if j % 256 < BOX:
            ztab[j, :G] = m[:, j % 256]
    mx = np.zeros((G, SX), np.float32)
    mx[:, :BOX] = m
    return ytab, ztab, mx


def split(v):
    hi = v.astype(BF16)
    return hi, (v - hi.astype(F32)).astype(BF16)


def dot(a, b):
    return jnp.dot(a, b, preferred_element_type=F32)


def kernel(
    pot, root, ytab_in, ztab_in, mxt_in, out,
    ytab, ztab, mxt, stage, roots, roots_s, xr, zsend, zrecv, e_ref, w_ref, my_ref, t1h, t1l, s_ref, fields, relay,
    table_sem, out_sem, ready, ready_z, root_send, root_recv, local_sem, own_sem, x_send, x_recv, xd_send, xd_recv,
    z_send, z_recv, zd_send, zd_recv, f_send, f_recv, r_send, r_recv,
):
    tables_in = [
        pltpu.make_async_copy(a, b, table_sem.at[i])
        for i, (a, b) in enumerate(((ytab_in, ytab), (ztab_in, ztab), (mxt_in, mxt), (root, roots.at[0])))
    ]
    me = lax.axis_index("gx")
    core = lax.axis_index("gy")
    plane = lax.axis_index("gz")
    my_y, my_x = me // 4, me % 4

    def line(g):
        return {"gx": g, "gy": core, "gz": plane}

    def shifted(k):
        return ((my_y + k // 4) % 4) * 4 + (my_x + k % 4) % 4

    nxt, prv = (me + 1) % GX, (me + GX - 1) % GX
    partner = {"gx": me, "gy": 1 - core, "gz": plane}
    z_up = {"gx": me, "gy": core, "gz": (plane + 1) % 4}
    z_down = {"gx": me, "gy": core, "gz": (plane + 3) % 4}

    barrier = pltpu.get_barrier_semaphore()
    first = [partner, z_up, z_down, line(nxt), line(prv)] + [line(shifted(k)) for k in (1, 2, 3, 4, 8, 12)]
    for d in first:
        pl.semaphore_signal(barrier, inc=1, device_id=d, device_id_type=MESH)
    mine = pl.ds(pl.multiple_of(core * 64, 64), BY)

    local = pltpu.make_async_copy(pot, xr.at[pl.ds(HALO, BX), mine], local_sem.at[0])
    local.start()
    lane = lax.broadcasted_iota(jnp.int32, (32, 128), 1)

    def pack(first, count, slab):
        @pl.loop(0, count)
        def _(u):
            for part in range(2):
                here = pl.ds(pl.multiple_of(core * 64 + 32 * part, 32), 32)
                tiles = [[jnp.zeros((32, 128), F32) for _ in range(2)] for _ in range(2)]
                for j, off in enumerate(OFFSETS):
                    v = xr[slab + 7 * u + j, here, :]
                    for d, at in enumerate((off - 94, off)):
                        w = pltpu.roll(v, at % 128, 1) if at % 128 else v
                        if j == 3:
                            tiles[d][0] = jnp.where(lane >= off, w, tiles[d][0])
                            tiles[d][1] = jnp.where(lane < off + 34 - 128, w, tiles[d][1])
                        else:
                            inside = (lane >= off) & (lane < off + 34)
                            tiles[d][j // 4] = jnp.where(inside, w, tiles[d][j // 4])
                for d in range(2):
                    for t in range(2):
                        zsend[d, 2 * (first + u) + t, 32 * part : 32 * part + 32] = tiles[d][t]

    def own_units(work):
        work(0, 8, 34)
        work(8, 1, 87)

    for c in tables_in:
        c.start()
    local.wait()
    own_units(pack)
    pack(17, 1, 87)
    pack(18, 1, 61)
    pl.semaphore_wait(barrier, len(first))
    for d in (z_up, z_down):
        pl.semaphore_signal(ready_z, inc=1, device_id=d, device_id_type=MESH)
    for k in (4, 8, 12):
        pl.semaphore_signal(ready, inc=1, device_id=line(shifted(k)), device_id_type=MESH)

    def remote(src, dst, ssem, rsem, to):
        return pltpu.make_async_remote_copy(
            src_ref=src, dst_ref=dst, send_sem=ssem, recv_sem=rsem, device_id=to, device_id_type=MESH
        )

    x_parts = (
        (26, 0, 14, nxt), (0, 94, 13, prv), (40, 14, 7, nxt), (13, 107, 7, prv),
        (47, 21, 7, nxt), (20, 114, 7, prv), (54, 28, 6, nxt), (27, 121, 7, prv),
    )
    x_copies = [
        remote(pot.at[pl.ds(s, n)], xr.at[pl.ds(e, n), mine], x_send.at[i], x_recv.at[i], line(to))
        for i, (s, e, n, to) in enumerate(x_parts)
    ]
    def root_copy(k):
        return remote(root, roots.at[k], root_send.at[k], root_recv.at[k], line(shifted(k)))

    for c in x_copies[:6]:
        c.start()
    own_d2d = remote(pot, xr.at[pl.ds(HALO, BX), mine], own_sem.at[0], own_sem.at[1], partner)
    own_d2d.start()

    def z_copies(i, first, count, line_to):
        rows = pl.ds(2 * first, 2 * count)
        return [
            remote(
                zsend.at[d, rows, 0:BY], zrecv.at[d, rows, mine], z_send.at[i, d], z_recv.at[i, d],
                {"gx": line_to, "gy": core, "gz": (plane + step) % 4},
            )
            for d, step in enumerate((1, 3))
        ]

    def z_relays(i, first, count):
        rows = pl.ds(2 * first, 2 * count)
        return [
            remote(zrecv.at[d, rows, mine], zrecv.at[d, rows, mine], zd_send.at[i, d], zd_recv.at[i, d], partner)
            for d in range(2)
        ]

    def x_relay(i):
        _, e, n, _ = x_parts[i]
        return remote(xr.at[pl.ds(e, n), mine], xr.at[pl.ds(e, n), mine], xd_send.at[i], xd_recv.at[i], partner)

    def convert_own(slab, count):
        @pl.loop(0, count // 2)
        def _(p):
            for j in range(2):
                x = slab + 2 * p + j
                h, l = split(xr[x])
                e_ref[x, 0:128, 0:128] = h
                e_ref[x, 128:256, 0:128] = l

    def convert_edges(first, count, slab):
        @pl.loop(0, count)
        def _(u):
            for part in range(4):
                here = pl.ds(32 * part, 32)
                below = [zrecv[0, 2 * (first + u) + t, here, :] for t in range(2)]
                above = [zrecv[1, 2 * (first + u) + t, here, :] for t in range(2)]
                for j, off in enumerate(OFFSETS):
                    x = slab + 7 * u + j
                    both = []
                    for tiles, at in ((above, -off), (below, 94 - off)):
                        v = jnp.where(lane >= off, tiles[0], tiles[1]) if j == 3 else tiles[j // 4]
                        both.append(pltpu.roll(v, at % 128, 1) if at % 128 else v)
                    h, l = split(jnp.where(lane < 34, both[0], jnp.where(lane >= 94, both[1], 0.0)))
                    e_ref[x, 32 * part : 32 * part + 32, 128:256] = h
                    e_ref[x, 128 + 32 * part : 160 + 32 * part, 128:256] = l

    z_parts = (
        (0, 9, 34), (9, 2, 0), (11, 2, 93), (13, 1, 14), (14, 1, 107), (15, 1, 21), (16, 1, 114),
        (17, 1, 27), (18, 1, 121),
    )
    z_all = [
        z_copies(i, f, n, me if i < 7 else nxt if i == 7 else prv) for i, (f, n, _) in enumerate(z_parts)
    ]
    relays = [z_relays(i, f, n) for i, (f, n, _) in enumerate(z_parts)]
    x_relays = [x_relay(i) for i in range(8)]

    def x_arrived(i):
        x_copies[i].wait_recv()
        x_relays[i].start()
        if i < 6:
            pack(*z_parts[i + 1])
            for c in z_all[i + 1]:
                c.start()

    def x_complete(i):
        x_relays[i].wait_recv()
        _, e, n, _ = x_parts[i]
        convert_own(e - n % 2, n + n % 2)

    def z_arrived(i):
        for d in range(2):
            z_all[i][d].wait_recv()
            relays[i][d].start()

    def z_complete(i):
        for d in range(2):
            relays[i][d].wait_recv()
        if i:
            convert_edges(*z_parts[i])
        else:
            own_units(convert_edges)

    for c in z_all[0]:
        c.start()

    pl.semaphore_wait(ready_z, 2)
    for c in z_all[7] + z_all[8] + x_copies[6:]:
        c.start()

    @pl.loop(0, EXT)
    def _(x):
        xr[x, 60:64, :] = jnp.zeros((4, 128), F32)
        xr[x, 124:128, :] = jnp.zeros((4, 128), F32)

    @pl.loop(0, 2 * UNITS)
    def _(t):
        for d in range(2):
            zrecv[d, t, 60:64, :] = jnp.zeros((4, 128), F32)
            zrecv[d, t, 124:128, :] = jnp.zeros((4, 128), F32)

    s_ref[...] = jnp.zeros(s_ref.shape, F32)
    pl.semaphore_wait(ready, 3)

    @pl.loop(1, GX)
    def _(k):
        root_copy(k).start()

    own_d2d.wait_recv()
    convert_own(HALO, BX)
    x_arrived(0)
    x_arrived(1)
    z_arrived(0)
    x_complete(0)
    x_complete(1)
    x_arrived(2)
    x_arrived(3)
    z_complete(0)
    z_arrived(1)
    z_arrived(2)
    x_complete(2)
    x_complete(3)
    x_arrived(4)
    x_arrived(5)
    z_complete(1)
    z_complete(2)
    z_arrived(3)
    z_arrived(4)
    x_complete(4)
    x_complete(5)
    z_complete(3)
    z_complete(4)
    z_arrived(7)
    z_arrived(8)
    z_arrived(5)
    z_arrived(6)
    x_arrived(6)
    x_arrived(7)
    z_complete(7)
    z_complete(8)
    @pl.loop(1, GX)
    def _(k):
        root_copy(k).wait_recv()

    for c in tables_in:
        c.wait()
    roots_copy = pltpu.make_async_copy(roots, roots_s, local_sem.at[1])
    roots_copy.start()
    z_complete(5)
    z_complete(6)
    x_complete(6)
    x_complete(7)
    roots_copy.wait()

    mx = mxt[...]
    roll_lane = lax.broadcasted_iota(jnp.int32, (SX, 128), 1)
    sent = pl.ds(0, SENT)
    relay_legs = {k: leg for k, leg, _ in RELAYED}

    def f_copy(i):
        k = ORDER[i]
        if k in relay_legs:
            j = [r[0] for r in RELAYED].index(k)
            return remote(fields.at[i, sent], relay.at[j], f_send.at[i], r_recv.at[j], line(shifted(relay_legs[k])))
        return remote(fields.at[i, sent], fields.at[GX + i, sent], f_send.at[i], f_recv.at[i], line(shifted(k)))

    def forward(j):
        k, _, leg = RELAYED[j]
        i = ORDER.index(k)
        return remote(relay.at[j], fields.at[GX + i, sent], r_send.at[j], f_recv.at[i], line(shifted(leg)))

    def arrival(i):
        return remote(fields.at[i, sent], fields.at[GX + i, sent], f_send.at[i], f_recv.at[i], line(shifted(1)))

    def choose(i, values):
        total = jnp.int32(0)
        for c, v in enumerate(values):
            total = jnp.where(i == c, v, total)
        return total

    def field(i):
        k = choose(i, ORDER)
        back = ((4 - k // 4) % 4) * 4 + (4 - k % 4) % 4
        rx, ry, rz = jnp.int32(0), jnp.int32(0), jnp.int32(0)
        for s in range(SLOTS):
            fx = roots_s[back, 0, s]
            mine_too = (fx + HALO) % NX // BX == me
            rx = jnp.where(mine_too, fx, rx)
            ry = jnp.where(mine_too, roots_s[back, 1, s], ry)
            rz = jnp.where(mine_too, roots_s[back, 2, s], rz)
        sx = jnp.minimum((rx + HALO - me * BX + NX) % NX, BX - 1)
        sy = ry
        sz = (rz - plane * BZ + NZ) % 256
        my_t = jnp.concatenate([ytab[pl.ds(NY - sy, 64), :], ytab[pl.ds(NY + BY - sy, 64), :]], axis=0)
        my_hi, my_lo = split(my_t.T[0:G, :])
        my_ref[0:G, 0:128] = my_hi
        my_ref[0:G, 128:256] = my_hi
        my_ref[G : 2 * G, 0:128] = my_lo
        my_ref[G : 2 * G, 128:256] = my_lo
        z_hi, z_lo = split(ztab[pl.ds(256 - sz, 256), :])
        w_ref[:, 0:128] = z_hi
        w_ref[:, 128:256] = z_lo

        both = my_ref[...]
        for g in range(BOX // GROUP):
            for j in range(GROUP):
                t = dot(both, e_ref[sx + GROUP * g + j])
                hi, lo = split(t[:G] + t[G:])
                rows = pl.ds((GROUP * g + j) * G, G)
                t1h[rows, :] = hi
                t1l[rows, :] = lo
            rows = pl.ds(GROUP * g * G, GROUP * G)
            q = dot(t1h[rows, :], w_ref[...])
            t = q[:, :128] + q[:, 128:] + dot(t1l[rows, :], w_ref[:, 0:128])
            for j in range(GROUP):
                s_ref[pl.ds(GROUP * g + j, G, stride=SX), :] = t[G * j : G * j + G]

        for g in range(6):
            tiles = [jnp.zeros((SX, 128), F32) for _ in range(3)]
            for b in range(8):
                off = 48 * b % 128
                at = 48 * b // 128
                v = s_ref[pl.ds((8 * g + b) * SX, SX), :]
                if off:
                    v = pltpu.roll(v, off, 1)
                if off + 48 > 128:
                    tiles[at] = tiles[at] + jnp.where(roll_lane >= off, v, 0.0)
                    tiles[at + 1] = tiles[at + 1] + jnp.where(roll_lane < off, v, 0.0)
                else:
                    tiles[at] = tiles[at] + v
            r = jnp.concatenate([jnp.concatenate(tiles, axis=1), jnp.zeros((8, 384), F32)], axis=0)
            hi, lo = split(r)
            o = dot(mx, jnp.concatenate([hi, lo], axis=0))
            o = o[:G] + o[G:]
            for t in range(3):
                fields[i, pl.ds(3 * g + t, G, stride=18), :] = o[:, 128 * t : 128 * t + 128]

    @pl.loop(0, GX)
    def _(i):
        field(i)
        for c in range(GX - 1):

            @pl.when(i == c)
            def _():
                f_copy(c).start()
                for j, at in enumerate(FORWARD):
                    if at == c:
                        f_copy(ORDER.index(RELAYED[j][0])).wait_recv()
                        forward(j).start()

    for i in range(GX - 1):
        arrival(i).wait_recv()

    places = []
    for s in range(SLOTS):
        anchor = (roots_s[0, 0, s] + HALO) % NX // BX
        k = ((my_y - anchor // 4 + 4) % 4) * 4 + (my_x - anchor % 4 + 4) % 4
        places.append(choose(k, [GX + ORDER.index(c) if c else ORDER.index(0) for c in range(GX)]))

    out_copies = []
    for c in range(4):
        n = 216 if c < 3 else 216 - PLANE
        for s, at in enumerate(places):
            stage[pl.ds(864 * c + s, n, stride=4), :] = fields[at, 216 * c : 216 * c + n]
            if c == 3:
                for r in range(PLANE):
                    even = fields[at, pl.ds(r, 24, stride=2 * PLANE), :]
                    odd = fields[at, pl.ds(r + PLANE, 23, stride=2 * PLANE), :]
                    last = jnp.sum(even, axis=0, keepdims=True) - jnp.sum(odd, axis=0, keepdims=True)
                    stage[pl.ds(4 * (SENT + r) + s, 1), :] = last
        rows = pl.ds(864 * c, 864)
        out_copies.append(pltpu.make_async_copy(stage.at[rows], out.at[rows], out_sem.at[c]))
        out_copies[c].start()

    for i in range(GX - 1):
        f_copy(i).wait_send()
    for j in range(len(RELAYED)):
        forward(j).wait_send()

    @pl.loop(1, GX)
    def _(k):
        root_copy(k).wait_send()

    for c in out_copies:
        c.wait()
    own_d2d.wait_send()
    for i in range(8):
        x_copies[i].wait_send()
        x_relays[i].wait_send()
    for i in range(9):
        for d in range(2):
            z_all[i][d].wait_send()
            relays[i][d].wait_send()


def body(potential, frag_root):
    ytab, ztab, mx = tables()
    mx = jnp.asarray(mx)
    mx_hi, mx_lo = split(mx)
    zero = jnp.zeros((G, 8), BF16)
    mxt = jnp.concatenate(
        [jnp.concatenate([m, zero, m, zero], axis=1) for m in (mx_hi, mx_lo)], axis=0
    )
    dma = pltpu.SemaphoreType.DMA
    out = pl.pallas_call(
        kernel,
        out_shape=jax.ShapeDtypeStruct((FLAT * SLOTS, 128), F32),
        in_specs=[pl.BlockSpec(memory_space=pl.ANY)] * 5,
        out_specs=pl.BlockSpec(memory_space=pl.ANY),
        scratch_shapes=[
            pltpu.VMEM((248, 128), F32),
            pltpu.VMEM((512, 128), F32),
            pltpu.VMEM(mxt.shape, BF16),
            pltpu.VMEM((FLAT * SLOTS, 128), F32),
            pltpu.VMEM((GX, 3, SLOTS), jnp.int32),
            pltpu.SMEM((GX, 3, SLOTS), jnp.int32),
            pltpu.VMEM((EXT, YL, 128), F32),
            pltpu.VMEM((2, 2 * UNITS, 64, 128), F32),
            pltpu.VMEM((2, 2 * UNITS, YL, 128), F32),
            pltpu.VMEM((EXT, 2 * YL, 256), BF16),
            pltpu.VMEM((256, 256), BF16),
            pltpu.VMEM((2 * G, 2 * YL), BF16),
            pltpu.VMEM((BOX * G, 256), BF16),
            pltpu.VMEM((BOX * G, 256), BF16),
            pltpu.VMEM((G * SX, 128), F32),
            pltpu.VMEM((2 * GX, FLAT, 128), F32),
            pltpu.VMEM((len(RELAYED), SENT, 128), F32),
            dma((4,)), dma((4,)),
            pltpu.SemaphoreType.REGULAR, pltpu.SemaphoreType.REGULAR, dma((GX,)), dma((GX,)), dma((2,)), dma((2,)),
            dma((8,)), dma((8,)), dma((8,)), dma((8,)),
            dma((9, 2)), dma((9, 2)), dma((9, 2)), dma((9, 2)),
            dma((GX,)), dma((GX,)), dma((4,)), dma((4,)),
        ],
        compiler_params=pltpu.CompilerParams(
            collective_id=0, has_side_effects=True, vmem_limit_bytes=66 * 1000 * 1000
        ),
    )(potential, frag_root, jnp.asarray(ytab), jnp.asarray(ztab), mxt)
    return out.reshape(FLAT, SLOTS, 128).transpose(1, 0, 2).reshape(SLOTS, FLAT * 128)


def solution(mesh):
    return jax.shard_map(
        body,
        mesh=mesh,
        in_specs=(P("gx", "gy", "gz"), P(None, ("gx", "gy", "gz"))),
        out_specs=P(("gx", "gy", "gz"), None),
        check_vma=False,
    )
```

```python
import functools

import jax
import jax.numpy as jnp
import numpy as np
from jax import lax
from jax.experimental import pallas as pl
from jax.experimental.pallas import tpu as pltpu
from jax.sharding import PartitionSpec as P

MESH = pl.DeviceIdType.MESH
G = 48
BOX = 68
HALO = 34
BX = 60
BY = 60
BZ = 128
NX = 960
NY = 120
NZ = 512
GX = 16
SLOTS = 4
EXT = 128
YL = 128
FLAT = 864
PLANE = 18
SENT = FLAT - PLANE
SX = 72
ORDER = (10, 6, 14, 9, 11, 5, 15, 7, 13, 2, 8, 1, 3, 4, 12, 0)
RELAYED = ((6, 5, 1), (14, 15, 3), (9, 5, 4), (11, 15, 12))
FORWARD = (7, 8, 9, 10)
GROUP = 17
UNITS = 19
OFFSETS = (0, 34, 68, 102, 8, 42, 76)
F32 = jnp.float32
BF16 = jnp.bfloat16


def interp_matrix():
    a = np.arange(G)[:, None]
    x = np.arange(BOX)[None, :]
    total = np.ones((G, BOX))
    for k in range(1, G // 2):
        total = total + 2.0 * np.cos(2.0 * np.pi * k * (a / G - x / BOX))
    return (total / BOX).astype(np.float32)


def tables():
    m = interp_matrix()
    ytab = np.zeros((248, 128), np.float32)
    for j in range(248):
        if j % NY < BOX:
            ytab[j, :G] = m[:, j % NY]
    ztab = np.zeros((512, 128), np.float32)
    for j in range(512):
        if j % 256 < BOX:
            ztab[j, :G] = m[:, j % 256]
    mx = np.zeros((G, SX), np.float32)
    mx[:, :BOX] = m
    return ytab, ztab, mx


def split(v):
    hi = v.astype(BF16)
    return hi, (v - hi.astype(F32)).astype(BF16)


def dot(a, b):
    return jnp.dot(a, b, preferred_element_type=F32)


def kernel(
    pot, root, ytab_in, ztab_in, mxt_in, out,
    ytab, ztab, mxt, stage, roots, roots_s, xr, zsend, zrecv, e_ref, w_ref, my_ref, t1h, t1l, s_ref, fields, relay,
    table_sem, out_sem, ready, ready_z, root_send, root_recv, local_sem, own_sem, x_send, x_recv, xd_send, xd_recv,
    z_send, z_recv, zd_send, zd_recv, f_send, f_recv, r_send, r_recv,
):
    tables_in = [
        pltpu.make_async_copy(a, b, table_sem.at[i])
        for i, (a, b) in enumerate(((ytab_in, ytab), (ztab_in, ztab), (mxt_in, mxt), (root, roots.at[0])))
    ]
    me = lax.axis_index("gx")
    core = lax.axis_index("gy")
    plane = lax.axis_index("gz")
    my_y, my_x = me // 4, me % 4

    def line(g):
        return {"gx": g, "gy": core, "gz": plane}

    def shifted(k):
        return ((my_y + k // 4) % 4) * 4 + (my_x + k % 4) % 4

    nxt, prv = (me + 1) % GX, (me + GX - 1) % GX
    partner = {"gx": me, "gy": 1 - core, "gz": plane}
    z_up = {"gx": me, "gy": core, "gz": (plane + 1) % 4}
    z_down = {"gx": me, "gy": core, "gz": (plane + 3) % 4}

    barrier = pltpu.get_barrier_semaphore()
    first = [partner, z_up, z_down, line(nxt), line(prv)] + [line(shifted(k)) for k in (1, 2, 3, 4, 8, 12)]
    for d in first:
        pl.semaphore_signal(barrier, inc=1, device_id=d, device_id_type=MESH)
    mine = pl.ds(pl.multiple_of(core * 64, 64), BY)

    local = pltpu.make_async_copy(pot, xr.at[pl.ds(HALO, BX), mine], local_sem.at[0])
    local.start()
    lane = lax.broadcasted_iota(jnp.int32, (32, 128), 1)

    def pack(first, count, slab):
        @pl.loop(0, count)
        def _(u):
            for part in range(2):
                here = pl.ds(pl.multiple_of(core * 64 + 32 * part, 32), 32)
                tiles = [[jnp.zeros((32, 128), F32) for _ in range(2)] for _ in range(2)]
                for j, off in enumerate(OFFSETS):
                    v = xr[slab + 7 * u + j, here, :]
                    w = pltpu.roll(v, off, 1) if off else v
                    if j == 3:
                        tiles[0][0] = jnp.where((lane >= 68) & (lane < 94), w, tiles[0][0])
                        tiles[0][1] = jnp.where((lane >= 94) & (lane < 102), w, tiles[0][1])
                        tiles[1][0] = jnp.where(lane >= 102, w, tiles[1][0])
                        tiles[1][1] = jnp.where(lane < 8, w, tiles[1][1])
                    else:
                        t = j // 4
                        tiles[0][t] = jnp.where((lane + 34 - off) % 128 < 34, w, tiles[0][t])
                        tiles[1][t] = jnp.where((lane >= off) & (lane < off + 34), w, tiles[1][t])
                for d in range(2):
                    for t in range(2):
                        zsend[d, 2 * (first + u) + t, 32 * part : 32 * part + 32] = tiles[d][t]

    def own_units(work):
        work(0, 8, 34)
        work(8, 1, 87)

    for c in tables_in:
        c.start()
    local.wait()
    own_units(pack)
    pack(17, 1, 87)
    pack(18, 1, 61)
    pl.semaphore_wait(barrier, len(first))
    for d in (z_up, z_down):
        pl.semaphore_signal(ready_z, inc=1, device_id=d, device_id_type=MESH)
    for k in (4, 8, 12):
        pl.semaphore_signal(ready, inc=1, device_id=line(shifted(k)), device_id_type=MESH)

    def remote(src, dst, ssem, rsem, to):
        return pltpu.make_async_remote_copy(
            src_ref=src, dst_ref=dst, send_sem=ssem, recv_sem=rsem, device_id=to, device_id_type=MESH
        )

    x_parts = (
        (26, 0, 14, nxt), (0, 94, 13, prv), (40, 14, 7, nxt), (13, 107, 7, prv),
        (47, 21, 7, nxt), (20, 114, 7, prv), (54, 28, 6, nxt), (27, 121, 7, prv),
    )
    x_copies = [
        remote(pot.at[pl.ds(s, n)], xr.at[pl.ds(e, n), mine], x_send.at[i], x_recv.at[i], line(to))
        for i, (s, e, n, to) in enumerate(x_parts)
    ]
    def root_copy(k):
        return remote(root, roots.at[k], root_send.at[k], root_recv.at[k], line(shifted(k)))

    for c in x_copies[:6]:
        c.start()
    own_d2d = remote(pot, xr.at[pl.ds(HALO, BX), mine], own_sem.at[0], own_sem.at[1], partner)
    own_d2d.start()

    def z_copies(i, first, count, line_to):
        rows = pl.ds(2 * first, 2 * count)
        return [
            remote(
                zsend.at[d, rows, 0:BY], zrecv.at[d, rows, mine], z_send.at[i, d], z_recv.at[i, d],
                {"gx": line_to, "gy": core, "gz": (plane + step) % 4},
            )
            for d, step in enumerate((1, 3))
        ]

    def z_relays(i, first, count):
        rows = pl.ds(2 * first, 2 * count)
        return [
            remote(zrecv.at[d, rows, mine], zrecv.at[d, rows, mine], zd_send.at[i, d], zd_recv.at[i, d], partner)
            for d in range(2)
        ]

    def x_relay(i):
        _, e, n, _ = x_parts[i]
        return remote(xr.at[pl.ds(e, n), mine], xr.at[pl.ds(e, n), mine], xd_send.at[i], xd_recv.at[i], partner)

    def convert_own(slab, count):
        @pl.loop(0, count // 2)
        def _(p):
            for j in range(2):
                x = slab + 2 * p + j
                h, l = split(xr[x])
                e_ref[x, 0:128, 0:128] = h
                e_ref[x, 128:256, 0:128] = l

    def convert_edges(first, count, slab):
        @pl.loop(0, count)
        def _(u):
            for part in range(4):
                here = pl.ds(32 * part, 32)
                below = [zrecv[0, 2 * (first + u) + t, here, :] for t in range(2)]
                above = [zrecv[1, 2 * (first + u) + t, here, :] for t in range(2)]
                for j, off in enumerate(OFFSETS):
                    x = slab + 7 * u + j
                    if j == 3:
                        v = jnp.where(lane < 94, below[0], below[1])
                        v = jnp.where(lane < 8, above[1], jnp.where(lane >= 102, above[0], v))
                    else:
                        v = jnp.where((lane >= off) & (lane < off + 34), above[j // 4], below[j // 4])
                    h, l = split(pltpu.roll(v, 128 - off, 1) if off else v)
                    e_ref[x, 32 * part : 32 * part + 32, 128:256] = h
                    e_ref[x, 128 + 32 * part : 160 + 32 * part, 128:256] = l

    z_parts = (
        (0, 9, 34), (9, 2, 0), (11, 2, 93), (13, 1, 14), (14, 1, 107), (15, 1, 21), (16, 1, 114),
        (17, 1, 27), (18, 1, 121),
    )
    z_all = [
        z_copies(i, f, n, me if i < 7 else nxt if i == 7 else prv) for i, (f, n, _) in enumerate(z_parts)
    ]
    relays = [z_relays(i, f, n) for i, (f, n, _) in enumerate(z_parts)]
    x_relays = [x_relay(i) for i in range(8)]

    def x_arrived(i):
        x_copies[i].wait_recv()
        x_relays[i].start()
        if i < 6:
            pack(*z_parts[i + 1])
            for c in z_all[i + 1]:
                c.start()

    def x_complete(i):
        x_relays[i].wait_recv()
        _, e, n, _ = x_parts[i]
        convert_own(e - n % 2, n + n % 2)

    def z_arrived(i):
        for d in range(2):
            z_all[i][d].wait_recv()
            relays[i][d].start()

    def z_complete(i):
        for d in range(2):
            relays[i][d].wait_recv()
        if i:
            convert_edges(*z_parts[i])
        else:
            own_units(convert_edges)

    for c in z_all[0]:
        c.start()

    pl.semaphore_wait(ready_z, 2)
    for c in z_all[7] + z_all[8] + x_copies[6:]:
        c.start()

    @pl.loop(0, EXT)
    def _(x):
        xr[x, 60:64, :] = jnp.zeros((4, 128), F32)
        xr[x, 124:128, :] = jnp.zeros((4, 128), F32)

    @pl.loop(0, 2 * UNITS)
    def _(t):
        for d in range(2):
            zrecv[d, t, 60:64, :] = jnp.zeros((4, 128), F32)
            zrecv[d, t, 124:128, :] = jnp.zeros((4, 128), F32)

    s_ref[...] = jnp.zeros(s_ref.shape, F32)
    pl.semaphore_wait(ready, 3)

    @pl.loop(1, GX)
    def _(k):
        root_copy(k).start()

    own_d2d.wait_recv()
    convert_own(HALO, BX)
    x_arrived(0)
    x_arrived(1)
    z_arrived(0)
    x_complete(0)
    x_complete(1)
    x_arrived(2)
    x_arrived(3)
    z_complete(0)
    z_arrived(1)
    z_arrived(2)
    x_complete(2)
    x_complete(3)
    x_arrived(4)
    x_arrived(5)
    z_complete(1)
    z_complete(2)
    z_arrived(3)
    z_arrived(4)
    x_complete(4)
    x_complete(5)
    z_complete(3)
    z_complete(4)
    z_arrived(7)
    z_arrived(8)
    z_arrived(5)
    z_arrived(6)
    x_arrived(6)
    x_arrived(7)
    z_complete(7)
    z_complete(8)
    @pl.loop(1, GX)
    def _(k):
        root_copy(k).wait_recv()

    for c in tables_in:
        c.wait()
    roots_copy = pltpu.make_async_copy(roots, roots_s, local_sem.at[1])
    roots_copy.start()
    z_complete(5)
    z_complete(6)
    x_complete(6)
    x_complete(7)
    roots_copy.wait()

    mx = mxt[...]
    roll_lane = lax.broadcasted_iota(jnp.int32, (SX, 128), 1)
    sent = pl.ds(0, SENT)
    relay_legs = {k: leg for k, leg, _ in RELAYED}

    def f_copy(i):
        k = ORDER[i]
        if k in relay_legs:
            j = [r[0] for r in RELAYED].index(k)
            return remote(fields.at[i, sent], relay.at[j], f_send.at[i], r_recv.at[j], line(shifted(relay_legs[k])))
        return remote(fields.at[i, sent], fields.at[GX + i, sent], f_send.at[i], f_recv.at[i], line(shifted(k)))

    def forward(j):
        k, _, leg = RELAYED[j]
        i = ORDER.index(k)
        return remote(relay.at[j], fields.at[GX + i, sent], r_send.at[j], f_recv.at[i], line(shifted(leg)))

    def arrival(i):
        return remote(fields.at[i, sent], fields.at[GX + i, sent], f_send.at[i], f_recv.at[i], line(shifted(1)))

    def choose(i, values):
        total = jnp.int32(0)
        for c, v in enumerate(values):
            total = jnp.where(i == c, v, total)
        return total

    def field(i):
        k = choose(i, ORDER)
        back = ((4 - k // 4) % 4) * 4 + (4 - k % 4) % 4
        rx, ry, rz = jnp.int32(0), jnp.int32(0), jnp.int32(0)
        for s in range(SLOTS):
            fx = roots_s[back, 0, s]
            mine_too = (fx + HALO) % NX // BX == me
            rx = jnp.where(mine_too, fx, rx)
            ry = jnp.where(mine_too, roots_s[back, 1, s], ry)
            rz = jnp.where(mine_too, roots_s[back, 2, s], rz)
        sx = jnp.minimum((rx + HALO - me * BX + NX) % NX, BX - 1)
        sy = ry
        sz = (rz - plane * BZ + NZ) % 256
        my_t = jnp.concatenate([ytab[pl.ds(NY - sy, 64), :], ytab[pl.ds(NY + BY - sy, 64), :]], axis=0)
        my_hi, my_lo = split(my_t.T[0:G, :])
        my_ref[0:G, 0:128] = my_hi
        my_ref[0:G, 128:256] = my_hi
        my_ref[G : 2 * G, 0:128] = my_lo
        my_ref[G : 2 * G, 128:256] = my_lo
        z_hi, z_lo = split(ztab[pl.ds(256 - sz, 256), :])
        w_ref[:, 0:128] = z_hi
        w_ref[:, 128:256] = z_lo

        both = my_ref[...]
        for g in range(BOX // GROUP):
            for j in range(GROUP):
                t = dot(both, e_ref[sx + GROUP * g + j])
                hi, lo = split(t[:G] + t[G:])
                rows = pl.ds((GROUP * g + j) * G, G)
                t1h[rows, :] = hi
                t1l[rows, :] = lo
            rows = pl.ds(GROUP * g * G, GROUP * G)
            q = dot(t1h[rows, :], w_ref[...])
            t = q[:, :128] + q[:, 128:] + dot(t1l[rows, :], w_ref[:, 0:128])
            for j in range(GROUP):
                s_ref[pl.ds(GROUP * g + j, G, stride=SX), :] = t[G * j : G * j + G]

        for g in range(6):
            tiles = [jnp.zeros((SX, 128), F32) for _ in range(3)]
            for b in range(8):
                off = 48 * b % 128
                at = 48 * b // 128
                v = s_ref[pl.ds((8 * g + b) * SX, SX), :]
                if off:
                    v = pltpu.roll(v, off, 1)
                if off + 48 > 128:
                    tiles[at] = tiles[at] + jnp.where(roll_lane >= off, v, 0.0)
                    tiles[at + 1] = tiles[at + 1] + jnp.where(roll_lane < off, v, 0.0)
                else:
                    tiles[at] = tiles[at] + v
            r = jnp.concatenate([jnp.concatenate(tiles, axis=1), jnp.zeros((8, 384), F32)], axis=0)
            hi, lo = split(r)
            o = dot(mx, jnp.concatenate([hi, lo], axis=0))
            o = o[:G] + o[G:]
            for t in range(3):
                fields[i, pl.ds(3 * g + t, G, stride=18), :] = o[:, 128 * t : 128 * t + 128]

    @pl.loop(0, GX)
    def _(i):
        field(i)
        for c in range(GX - 1):

            @pl.when(i == c)
            def _():
                f_copy(c).start()
                for j, at in enumerate(FORWARD):
                    if at == c:
                        f_copy(ORDER.index(RELAYED[j][0])).wait_recv()
                        forward(j).start()

    for i in range(GX - 1):
        arrival(i).wait_recv()

    places = []
    for s in range(SLOTS):
        anchor = (roots_s[0, 0, s] + HALO) % NX // BX
        k = ((my_y - anchor // 4 + 4) % 4) * 4 + (my_x - anchor % 4 + 4) % 4
        places.append(choose(k, [GX + ORDER.index(c) if c else ORDER.index(0) for c in range(GX)]))

    out_copies = []
    for c in range(4):
        n = 216 if c < 3 else 216 - PLANE
        for s, at in enumerate(places):
            stage[pl.ds(864 * c + s, n, stride=4), :] = fields[at, 216 * c : 216 * c + n]
            if c == 3:
                for r in range(PLANE):
                    even = fields[at, pl.ds(r, 24, stride=2 * PLANE), :]
                    odd = fields[at, pl.ds(r + PLANE, 23, stride=2 * PLANE), :]
                    last = jnp.sum(even, axis=0, keepdims=True) - jnp.sum(odd, axis=0, keepdims=True)
                    stage[pl.ds(4 * (SENT + r) + s, 1), :] = last
        rows = pl.ds(864 * c, 864)
        out_copies.append(pltpu.make_async_copy(stage.at[rows], out.at[rows], out_sem.at[c]))
        out_copies[c].start()

    for i in range(GX - 1):
        f_copy(i).wait_send()
    for j in range(len(RELAYED)):
        forward(j).wait_send()

    @pl.loop(1, GX)
    def _(k):
        root_copy(k).wait_send()

    for c in out_copies:
        c.wait()
    own_d2d.wait_send()
    for i in range(8):
        x_copies[i].wait_send()
        x_relays[i].wait_send()
    for i in range(9):
        for d in range(2):
            z_all[i][d].wait_send()
            relays[i][d].wait_send()


def body(potential, frag_root):
    ytab, ztab, mx = tables()
    mx = jnp.asarray(mx)
    mx_hi, mx_lo = split(mx)
    zero = jnp.zeros((G, 8), BF16)
    mxt = jnp.concatenate(
        [jnp.concatenate([m, zero, m, zero], axis=1) for m in (mx_hi, mx_lo)], axis=0
    )
    dma = pltpu.SemaphoreType.DMA
    out = pl.pallas_call(
        kernel,
        out_shape=jax.ShapeDtypeStruct((FLAT * SLOTS, 128), F32),
        in_specs=[pl.BlockSpec(memory_space=pl.ANY)] * 5,
        out_specs=pl.BlockSpec(memory_space=pl.ANY),
        scratch_shapes=[
            pltpu.VMEM((248, 128), F32),
            pltpu.VMEM((512, 128), F32),
            pltpu.VMEM(mxt.shape, BF16),
            pltpu.VMEM((FLAT * SLOTS, 128), F32),
            pltpu.VMEM((GX, 3, SLOTS), jnp.int32),
            pltpu.SMEM((GX, 3, SLOTS), jnp.int32),
            pltpu.VMEM((EXT, YL, 128), F32),
            pltpu.VMEM((2, 2 * UNITS, 64, 128), F32),
            pltpu.VMEM((2, 2 * UNITS, YL, 128), F32),
            pltpu.VMEM((EXT, 2 * YL, 256), BF16),
            pltpu.VMEM((256, 256), BF16),
            pltpu.VMEM((2 * G, 2 * YL), BF16),
            pltpu.VMEM((BOX * G, 256), BF16),
            pltpu.VMEM((BOX * G, 256), BF16),
            pltpu.VMEM((G * SX, 128), F32),
            pltpu.VMEM((2 * GX, FLAT, 128), F32),
            pltpu.VMEM((len(RELAYED), SENT, 128), F32),
            dma((4,)), dma((4,)),
            pltpu.SemaphoreType.REGULAR, pltpu.SemaphoreType.REGULAR, dma((GX,)), dma((GX,)), dma((2,)), dma((2,)),
            dma((8,)), dma((8,)), dma((8,)), dma((8,)),
            dma((9, 2)), dma((9, 2)), dma((9, 2)), dma((9, 2)),
            dma((GX,)), dma((GX,)), dma((4,)), dma((4,)),
        ],
        compiler_params=pltpu.CompilerParams(
            collective_id=0, has_side_effects=True, vmem_limit_bytes=66 * 1000 * 1000
        ),
    )(potential, frag_root, jnp.asarray(ytab), jnp.asarray(ztab), mxt)
    return out.reshape(FLAT, SLOTS, 128).transpose(1, 0, 2).reshape(SLOTS, FLAT * 128)


def solution(mesh):
    return jax.shard_map(
        body,
        mesh=mesh,
        in_specs=(P("gx", "gy", "gz"), P(None, ("gx", "gy", "gz"))),
        out_specs=P(("gx", "gy", "gz"), None),
        check_vma=False,
    )
```

```python
import functools

import jax
import jax.numpy as jnp
import numpy as np
from jax import lax
from jax.experimental import pallas as pl
from jax.experimental.pallas import tpu as pltpu
from jax.sharding import PartitionSpec as P

MESH = pl.DeviceIdType.MESH
G = 48
BOX = 68
HALO = 34
BX = 60
BY = 60
BZ = 128
NX = 960
NY = 120
NZ = 512
GX = 16
SLOTS = 4
EXT = 128
YL = 128
FLAT = 864
PLANE = 18
SENT = FLAT - PLANE
SX = 72
ORDER = (10, 6, 14, 9, 11, 5, 15, 7, 13, 2, 8, 1, 3, 4, 12, 0)
RELAYED = ((6, 5, 1), (14, 15, 3), (9, 5, 4), (11, 15, 12))
FORWARD = (7, 8, 9, 10)
GROUP = 17
UNITS = 19
OFFSETS = (0, 34, 68, 102, 8, 42, 76)
F32 = jnp.float32
BF16 = jnp.bfloat16


def interp_matrix():
    a = np.arange(G)[:, None]
    x = np.arange(BOX)[None, :]
    total = np.ones((G, BOX))
    for k in range(1, G // 2):
        total = total + 2.0 * np.cos(2.0 * np.pi * k * (a / G - x / BOX))
    return (total / BOX).astype(np.float32)


def tables():
    m = interp_matrix()
    ytab = np.zeros((248, 128), np.float32)
    for j in range(248):
        if j % NY < BOX:
            ytab[j, :G] = m[:, j % NY]
    ztab = np.zeros((512, 128), np.float32)
    for j in range(512):
        if j % 256 < BOX:
            ztab[j, :G] = m[:, j % 256]
    mx = np.zeros((G, SX), np.float32)
    mx[:, :BOX] = m
    return ytab, ztab, mx


def split(v):
    hi = v.astype(BF16)
    return hi, (v - hi.astype(F32)).astype(BF16)


def dot(a, b):
    return jnp.dot(a, b, preferred_element_type=F32)


def kernel(
    pot, root, ytab_in, ztab_in, mxt_in, out,
    ytab, ztab, mxt, stage, roots, roots_s, xr, zsend, zrecv, e_ref, w_ref, my_ref, t1h, t1l, s_ref, fields, relay,
    table_sem, out_sem, ready, ready_z, root_send, root_recv, local_sem, own_sem, x_send, x_recv, xd_send, xd_recv,
    z_send, z_recv, zd_send, zd_recv, f_send, f_recv, r_send, r_recv,
):
    tables_in = [
        pltpu.make_async_copy(a, b, table_sem.at[i])
        for i, (a, b) in enumerate(((ytab_in, ytab), (ztab_in, ztab), (mxt_in, mxt), (root, roots.at[0])))
    ]
    me = lax.axis_index("gx")
    core = lax.axis_index("gy")
    plane = lax.axis_index("gz")
    my_y, my_x = me // 4, me % 4

    def line(g):
        return {"gx": g, "gy": core, "gz": plane}

    def shifted(k):
        return ((my_y + k // 4) % 4) * 4 + (my_x + k % 4) % 4

    nxt, prv = (me + 1) % GX, (me + GX - 1) % GX
    partner = {"gx": me, "gy": 1 - core, "gz": plane}
    z_up = {"gx": me, "gy": core, "gz": (plane + 1) % 4}
    z_down = {"gx": me, "gy": core, "gz": (plane + 3) % 4}

    barrier = pltpu.get_barrier_semaphore()
    first = [partner, z_up, z_down, line(nxt), line(prv)] + [line(shifted(k)) for k in (1, 2, 3, 4, 8, 12)]
    for d in first:
        pl.semaphore_signal(barrier, inc=1, device_id=d, device_id_type=MESH)
    mine = pl.ds(pl.multiple_of(core * 64, 64), BY)

    local = pltpu.make_async_copy(pot, xr.at[pl.ds(HALO, BX), mine], local_sem.at[0])
    local.start()
    lane = lax.broadcasted_iota(jnp.int32, (32, 128), 1)

    def pack(first, count, slab):
        @pl.loop(0, count)
        def _(u):
            for part in range(2):
                here = pl.ds(pl.multiple_of(core * 64 + 32 * part, 32), 32)
                tiles = [[jnp.zeros((32, 128), F32) for _ in range(2)] for _ in range(2)]
                for j, off in enumerate(OFFSETS):
                    v = xr[slab + 7 * u + j, here, :]
                    w = pltpu.roll(v, off, 1) if off else v
                    if j == 3:
                        tiles[0][0] = jnp.where((lane >= 68) & (lane < 94), w, tiles[0][0])
                        tiles[0][1] = jnp.where((lane >= 94) & (lane < 102), w, tiles[0][1])
                        tiles[1][0] = jnp.where(lane >= 102, w, tiles[1][0])
                        tiles[1][1] = jnp.where(lane < 8, w, tiles[1][1])
                    else:
                        t = j // 4
                        tiles[0][t] = jnp.where((lane + 34 - off) % 128 < 34, w, tiles[0][t])
                        tiles[1][t] = jnp.where((lane >= off) & (lane < off + 34), w, tiles[1][t])
                for d in range(2):
                    for t in range(2):
                        zsend[d, 2 * (first + u) + t, 32 * part : 32 * part + 32] = tiles[d][t]

    def own_units(work):
        work(0, 8, 34)
        work(8, 1, 87)

    for c in tables_in:
        c.start()
    local.wait()
    own_units(pack)
    pack(17, 1, 87)
    pack(18, 1, 61)
    pl.semaphore_wait(barrier, len(first))
    for d in (z_up, z_down):
        pl.semaphore_signal(ready_z, inc=1, device_id=d, device_id_type=MESH)
    for k in (4, 8, 12):
        pl.semaphore_signal(ready, inc=1, device_id=line(shifted(k)), device_id_type=MESH)

    def remote(src, dst, ssem, rsem, to):
        return pltpu.make_async_remote_copy(
            src_ref=src, dst_ref=dst, send_sem=ssem, recv_sem=rsem, device_id=to, device_id_type=MESH
        )

    x_parts = (
        (26, 0, 14, nxt), (0, 94, 13, prv), (40, 14, 7, nxt), (13, 107, 7, prv),
        (47, 21, 7, nxt), (20, 114, 7, prv), (54, 28, 6, nxt), (27, 121, 7, prv),
    )
    x_copies = [
        remote(pot.at[pl.ds(s, n)], xr.at[pl.ds(e, n), mine], x_send.at[i], x_recv.at[i], line(to))
        for i, (s, e, n, to) in enumerate(x_parts)
    ]
    def root_copy(k):
        return remote(root, roots.at[k], root_send.at[k], root_recv.at[k], line(shifted(k)))

    for c in x_copies[:6]:
        c.start()
    own_d2d = remote(pot, xr.at[pl.ds(HALO, BX), mine], own_sem.at[0], own_sem.at[1], partner)
    own_d2d.start()

    def z_copies(i, first, count, line_to):
        rows = pl.ds(2 * first, 2 * count)
        return [
            remote(
                zsend.at[d, rows, 0:BY], zrecv.at[d, rows, mine], z_send.at[i, d], z_recv.at[i, d],
                {"gx": line_to, "gy": core, "gz": (plane + step) % 4},
            )
            for d, step in enumerate((1, 3))
        ]

    def z_relays(i, first, count):
        rows = pl.ds(2 * first, 2 * count)
        return [
            remote(zrecv.at[d, rows, mine], zrecv.at[d, rows, mine], zd_send.at[i, d], zd_recv.at[i, d], partner)
            for d in range(2)
        ]

    def x_relay(i):
        _, e, n, _ = x_parts[i]
        return remote(xr.at[pl.ds(e, n), mine], xr.at[pl.ds(e, n), mine], xd_send.at[i], xd_recv.at[i], partner)

    def convert_own(slab, count):
        @pl.loop(0, count // 2)
        def _(p):
            for j in range(2):
                x = slab + 2 * p + j
                h, l = split(xr[x])
                e_ref[x, 0:128, 0:128] = h
                e_ref[x, 128:256, 0:128] = l

    def convert_edges(first, count, slab):
        @pl.loop(0, count)
        def _(u):
            for part in range(4):
                here = pl.ds(32 * part, 32)
                below = [zrecv[0, 2 * (first + u) + t, here, :] for t in range(2)]
                above = [zrecv[1, 2 * (first + u) + t, here, :] for t in range(2)]
                for j, off in enumerate(OFFSETS):
                    x = slab + 7 * u + j
                    if j == 3:
                        v = jnp.where(lane < 94, below[0], below[1])
                        v = jnp.where(lane < 8, above[1], jnp.where(lane >= 102, above[0], v))
                    else:
                        v = jnp.where((lane >= off) & (lane < off + 34), above[j // 4], below[j // 4])
                    h, l = split(pltpu.roll(v, 128 - off, 1) if off else v)
                    e_ref[x, 32 * part : 32 * part + 32, 128:256] = h
                    e_ref[x, 128 + 32 * part : 160 + 32 * part, 128:256] = l

    z_parts = (
        (0, 9, 34), (9, 2, 0), (11, 2, 93), (13, 1, 14), (14, 1, 107), (15, 1, 21), (16, 1, 114),
        (17, 1, 27), (18, 1, 121),
    )
    z_all = [
        z_copies(i, f, n, me if i < 7 else nxt if i == 7 else prv) for i, (f, n, _) in enumerate(z_parts)
    ]
    relays = [z_relays(i, f, n) for i, (f, n, _) in enumerate(z_parts)]
    x_relays = [x_relay(i) for i in range(8)]

    def x_arrived(i):
        x_copies[i].wait_recv()
        x_relays[i].start()
        if i < 6:
            pack(*z_parts[i + 1])
            for c in z_all[i + 1]:
                c.start()

    def x_complete(i):
        x_relays[i].wait_recv()
        _, e, n, _ = x_parts[i]
        convert_own(e - n % 2, n + n % 2)

    def z_arrived(i):
        for d in range(2):
            z_all[i][d].wait_recv()
            relays[i][d].start()

    def z_complete(i):
        for d in range(2):
            relays[i][d].wait_recv()
        if i:
            convert_edges(*z_parts[i])
        else:
            own_units(convert_edges)

    for c in z_all[0]:
        c.start()

    pl.semaphore_wait(ready, 3)

    @pl.loop(1, GX)
    def _(k):
        root_copy(k).start()

    pl.semaphore_wait(ready_z, 2)
    for c in z_all[7] + z_all[8] + x_copies[6:]:
        c.start()

    @pl.loop(0, EXT)
    def _(x):
        xr[x, 60:64, :] = jnp.zeros((4, 128), F32)
        xr[x, 124:128, :] = jnp.zeros((4, 128), F32)

    @pl.loop(0, 2 * UNITS)
    def _(t):
        for d in range(2):
            zrecv[d, t, 60:64, :] = jnp.zeros((4, 128), F32)
            zrecv[d, t, 124:128, :] = jnp.zeros((4, 128), F32)

    s_ref[...] = jnp.zeros(s_ref.shape, F32)
    own_d2d.wait_recv()
    convert_own(HALO, BX)
    x_arrived(0)
    x_arrived(1)
    z_arrived(0)
    x_complete(0)
    x_complete(1)
    x_arrived(2)
    x_arrived(3)
    z_complete(0)
    z_arrived(1)
    z_arrived(2)
    x_complete(2)
    x_complete(3)
    x_arrived(4)
    x_arrived(5)
    z_complete(1)
    z_complete(2)
    z_arrived(3)
    z_arrived(4)
    x_complete(4)
    x_complete(5)
    z_complete(3)
    z_complete(4)
    z_arrived(7)
    z_arrived(8)
    z_arrived(5)
    z_arrived(6)
    @pl.loop(1, GX)
    def _(k):
        root_copy(k).wait_recv()

    for c in tables_in:
        c.wait()
    roots_copy = pltpu.make_async_copy(roots, roots_s, local_sem.at[1])
    roots_copy.start()
    x_arrived(6)
    x_arrived(7)
    z_complete(7)
    z_complete(8)
    z_complete(5)
    z_complete(6)
    x_complete(6)
    x_complete(7)
    roots_copy.wait()

    mx = mxt[...]
    roll_lane = lax.broadcasted_iota(jnp.int32, (SX, 128), 1)
    sent = pl.ds(0, SENT)
    relay_legs = {k: leg for k, leg, _ in RELAYED}

    def f_copy(i):
        k = ORDER[i]
        if k in relay_legs:
            j = [r[0] for r in RELAYED].index(k)
            return remote(fields.at[i, sent], relay.at[j], f_send.at[i], r_recv.at[j], line(shifted(relay_legs[k])))
        return remote(fields.at[i, sent], fields.at[GX + i, sent], f_send.at[i], f_recv.at[i], line(shifted(k)))

    def forward(j):
        k, _, leg = RELAYED[j]
        i = ORDER.index(k)
        return remote(relay.at[j], fields.at[GX + i, sent], r_send.at[j], f_recv.at[i], line(shifted(leg)))

    def arrival(i):
        return remote(fields.at[i, sent], fields.at[GX + i, sent], f_send.at[i], f_recv.at[i], line(shifted(1)))

    def choose(i, values):
        total = jnp.int32(0)
        for c, v in enumerate(values):
            total = jnp.where(i == c, v, total)
        return total

    def field(i):
        k = choose(i, ORDER)
        back = ((4 - k // 4) % 4) * 4 + (4 - k % 4) % 4
        rx, ry, rz = jnp.int32(0), jnp.int32(0), jnp.int32(0)
        for s in range(SLOTS):
            fx = roots_s[back, 0, s]
            mine_too = (fx + HALO) % NX // BX == me
            rx = jnp.where(mine_too, fx, rx)
            ry = jnp.where(mine_too, roots_s[back, 1, s], ry)
            rz = jnp.where(mine_too, roots_s[back, 2, s], rz)
        sx = jnp.minimum((rx + HALO - me * BX + NX) % NX, BX - 1)
        sy = ry
        sz = (rz - plane * BZ + NZ) % 256
        my_t = jnp.concatenate([ytab[pl.ds(NY - sy, 64), :], ytab[pl.ds(NY + BY - sy, 64), :]], axis=0)
        my_hi, my_lo = split(my_t.T[0:G, :])
        my_ref[0:G, 0:128] = my_hi
        my_ref[0:G, 128:256] = my_hi
        my_ref[G : 2 * G, 0:128] = my_lo
        my_ref[G : 2 * G, 128:256] = my_lo
        z_hi, z_lo = split(ztab[pl.ds(256 - sz, 256), :])
        w_ref[:, 0:128] = z_hi
        w_ref[:, 128:256] = z_lo

        both = my_ref[...]
        for g in range(BOX // GROUP):
            for j in range(GROUP):
                t = dot(both, e_ref[sx + GROUP * g + j])
                hi, lo = split(t[:G] + t[G:])
                rows = pl.ds((GROUP * g + j) * G, G)
                t1h[rows, :] = hi
                t1l[rows, :] = lo
            rows = pl.ds(GROUP * g * G, GROUP * G)
            q = dot(t1h[rows, :], w_ref[...])
            t = q[:, :128] + q[:, 128:] + dot(t1l[rows, :], w_ref[:, 0:128])
            for j in range(GROUP):
                s_ref[pl.ds(GROUP * g + j, G, stride=SX), :] = t[G * j : G * j + G]

        for g in range(6):
            tiles = [jnp.zeros((SX, 128), F32) for _ in range(3)]
            for b in range(8):
                off = 48 * b % 128
                at = 48 * b // 128
                v = s_ref[pl.ds((8 * g + b) * SX, SX), :]
                if off:
                    v = pltpu.roll(v, off, 1)
                if off + 48 > 128:
                    tiles[at] = tiles[at] + jnp.where(roll_lane >= off, v, 0.0)
                    tiles[at + 1] = tiles[at + 1] + jnp.where(roll_lane < off, v, 0.0)
                else:
                    tiles[at] = tiles[at] + v
            r = jnp.concatenate([jnp.concatenate(tiles, axis=1), jnp.zeros((8, 384), F32)], axis=0)
            hi, lo = split(r)
            o = dot(mx, jnp.concatenate([hi, lo], axis=0))
            o = o[:G] + o[G:]
            for t in range(3):
                fields[i, pl.ds(3 * g + t, G, stride=18), :] = o[:, 128 * t : 128 * t + 128]

    @pl.loop(0, GX)
    def _(i):
        field(i)
        for c in range(GX - 1):

            @pl.when(i == c)
            def _():
                f_copy(c).start()
                for j, at in enumerate(FORWARD):
                    if at == c:
                        f_copy(ORDER.index(RELAYED[j][0])).wait_recv()
                        forward(j).start()

    for i in range(GX - 1):
        arrival(i).wait_recv()

    places = []
    for s in range(SLOTS):
        anchor = (roots_s[0, 0, s] + HALO) % NX // BX
        k = ((my_y - anchor // 4 + 4) % 4) * 4 + (my_x - anchor % 4 + 4) % 4
        places.append(choose(k, [GX + ORDER.index(c) if c else ORDER.index(0) for c in range(GX)]))

    out_copies = []
    for c in range(4):
        n = 216 if c < 3 else 216 - PLANE
        for s, at in enumerate(places):
            stage[pl.ds(864 * c + s, n, stride=4), :] = fields[at, 216 * c : 216 * c + n]
            if c == 3:
                for r in range(PLANE):
                    even = fields[at, pl.ds(r, 24, stride=2 * PLANE), :]
                    odd = fields[at, pl.ds(r + PLANE, 23, stride=2 * PLANE), :]
                    last = jnp.sum(even, axis=0, keepdims=True) - jnp.sum(odd, axis=0, keepdims=True)
                    stage[pl.ds(4 * (SENT + r) + s, 1), :] = last
        rows = pl.ds(864 * c, 864)
        out_copies.append(pltpu.make_async_copy(stage.at[rows], out.at[rows], out_sem.at[c]))
        out_copies[c].start()

    for i in range(GX - 1):
        f_copy(i).wait_send()
    for j in range(len(RELAYED)):
        forward(j).wait_send()

    @pl.loop(1, GX)
    def _(k):
        root_copy(k).wait_send()

    for c in out_copies:
        c.wait()
    own_d2d.wait_send()
    for i in range(8):
        x_copies[i].wait_send()
        x_relays[i].wait_send()
    for i in range(9):
        for d in range(2):
            z_all[i][d].wait_send()
            relays[i][d].wait_send()


def body(potential, frag_root):
    ytab, ztab, mx = tables()
    mx = jnp.asarray(mx)
    mx_hi, mx_lo = split(mx)
    zero = jnp.zeros((G, 8), BF16)
    mxt = jnp.concatenate(
        [jnp.concatenate([m, zero, m, zero], axis=1) for m in (mx_hi, mx_lo)], axis=0
    )
    dma = pltpu.SemaphoreType.DMA
    out = pl.pallas_call(
        kernel,
        out_shape=jax.ShapeDtypeStruct((FLAT * SLOTS, 128), F32),
        in_specs=[pl.BlockSpec(memory_space=pl.ANY)] * 5,
        out_specs=pl.BlockSpec(memory_space=pl.ANY),
        scratch_shapes=[
            pltpu.VMEM((248, 128), F32),
            pltpu.VMEM((512, 128), F32),
            pltpu.VMEM(mxt.shape, BF16),
            pltpu.VMEM((FLAT * SLOTS, 128), F32),
            pltpu.VMEM((GX, 3, SLOTS), jnp.int32),
            pltpu.SMEM((GX, 3, SLOTS), jnp.int32),
            pltpu.VMEM((EXT, YL, 128), F32),
            pltpu.VMEM((2, 2 * UNITS, 64, 128), F32),
            pltpu.VMEM((2, 2 * UNITS, YL, 128), F32),
            pltpu.VMEM((EXT, 2 * YL, 256), BF16),
            pltpu.VMEM((256, 256), BF16),
            pltpu.VMEM((2 * G, 2 * YL), BF16),
            pltpu.VMEM((BOX * G, 256), BF16),
            pltpu.VMEM((BOX * G, 256), BF16),
            pltpu.VMEM((G * SX, 128), F32),
            pltpu.VMEM((2 * GX, FLAT, 128), F32),
            pltpu.VMEM((len(RELAYED), SENT, 128), F32),
            dma((4,)), dma((4,)),
            pltpu.SemaphoreType.REGULAR, pltpu.SemaphoreType.REGULAR, dma((GX,)), dma((GX,)), dma((2,)), dma((2,)),
            dma((8,)), dma((8,)), dma((8,)), dma((8,)),
            dma((9, 2)), dma((9, 2)), dma((9, 2)), dma((9, 2)),
            dma((GX,)), dma((GX,)), dma((4,)), dma((4,)),
        ],
        compiler_params=pltpu.CompilerParams(
            collective_id=0, has_side_effects=True, vmem_limit_bytes=66 * 1000 * 1000
        ),
    )(potential, frag_root, jnp.asarray(ytab), jnp.asarray(ztab), mxt)
    return out.reshape(FLAT, SLOTS, 128).transpose(1, 0, 2).reshape(SLOTS, FLAT * 128)


def solution(mesh):
    return jax.shard_map(
        body,
        mesh=mesh,
        in_specs=(P("gx", "gy", "gz"), P(None, ("gx", "gy", "gz"))),
        out_specs=P(("gx", "gy", "gz"), None),
        check_vma=False,
    )
```
